32 devices in a mesh: section: 2 (over core), dp: 4 (over z), tensor: 4 (over y, x).
Axes of the slice: x: 2, y: 2, z: 4, core: 2. Of those that a mesh axis runs over, the one named last changes fastest.
Arguments:
- inputs: bfloat16 [2, 512, 4096], P(None, 'dp', 'tensor'), may hold values from -6 to 6
- adapter_down: bfloat16 [2, 4096, 128], P('section', 'tensor'), may hold values from -0.09375 to 0.09375
- adapter_up: bfloat16 [2, 128, 4096], P('section', None, 'tensor'), may hold values from -0.5 to 0.5
- gains: bfloat16 [2, 4096], P('section', 'tensor'), may hold values from 0.25 to 1.75
- head: bfloat16 [4096, 128], P('tensor'), may hold values from -0.375 to 0.375
- labels: int32 [2, 512], P(None, 'dp'), may hold values from 0 to 127
- valid: int32 [2, 512], P(None, 'dp'), may hold values from 0 to 1, as said below
Outputs:
- grads_down: float32 [2, 4096, 128], P('section', 'tensor', 'dp')
- grads_up: float32 [2, 128, 4096], P('section', 'dp', 'tensor')
- grads_gain: float32 [2, 4096], P('section', 'tensor')
The draws below stay inside these ranges and needn't reach their ends.
Inputs may be any that keep to these rules, and one draw needn't show every extreme that they name: In each microbatch the first of every 128 consecutive tokens is valid.
All inputs are finite; a program needn't handle non-finite values.
Results may differ from the reference program's by a relative error of at most 0.015.
Values may be sent and summed in bfloat16 or wider, within the bound.
A program may use at most 64 MiB of HBM per device.

```python
import jax
import jax.numpy as jnp
from jax import lax

D = 4096
RANK = 128
LABELS = 128
TOK_DEV = 128
MICRO = 2
SECTIONS = 2
TOKENS = 512


def draw_valid(key, part):
    column = jnp.arange(TOKENS, dtype=jnp.int32)
    replica = column // TOK_DEV
    groups = TOKENS // TOK_DEV
    threshold = 256 + 512 * replica // max(groups - 1, 1)
    random_bits = jax.random.randint(key, (MICRO, TOKENS), 0, 1024, dtype=jnp.int32)
    chosen = (random_bits < threshold[None, :]) | (column % TOK_DEV == 0)[None, :]
    return chosen.astype(jnp.int32)


def with_ends(values, stream_key, smallest, top_value):
    spot = [jax.random.randint(jax.random.fold_in(stream_key, axis), (), 0, length) for axis, length in enumerate(values.shape)]
    main_axis = values.shape.index(max(values.shape))
    beside = spot[:main_axis] + [(spot[main_axis] + 1) % values.shape[main_axis]] + spot[main_axis + 1:]
    return values.at[tuple(spot)].set(smallest).at[tuple(beside)].set(top_value)


def block_levels(own_key, dims, cuts, low, largest):
    gain = 1.0
    for axis_at, shards_of in cuts:
        steps = jax.random.uniform(jax.random.fold_in(jax.random.fold_in(own_key, 6), axis_at), (shards_of,), jnp.float32, low / len(cuts), largest / len(cuts))
        gain = gain * jnp.repeat(jnp.exp(steps), dims[axis_at] // shards_of).reshape((-1,) + (1,) * (len(dims) - 1 - axis_at))
    return gain


def centred(own_key, extent, width, reach, pieces=(), held_as=jnp.bfloat16):
    entries = jax.random.normal(own_key, extent, jnp.float32) * width
    if len(pieces) > 0:
        entries = block_levels(own_key, extent, pieces, -0.22, 0.18) * entries
    return jnp.clip(entries, min=-reach, max=reach).astype(held_as)


def setup_inputs(seed: int = 0) -> dict:
    key_list = jax.random.split(jax.random.key(seed), 8)
    inputs = centred(key_list[0], (MICRO, TOKENS, D), 1.0, 6.0, ((1, 4), (2, 4)))
    adapter_down = centred(key_list[1], (SECTIONS, D, RANK), D ** -0.5, 0.09375, ((0, 2), (1, 4)))
    adapter_up = centred(key_list[2], (SECTIONS, RANK, D), RANK ** -0.5, 0.5, ((0, 2), (2, 4)))
    gains = jnp.clip(1.0 + 0.15 * jax.random.normal(key_list[3], (SECTIONS, D), jnp.float32), 0.25, 1.75).astype(jnp.bfloat16)
    head = centred(key_list[4], (D, LABELS), (D // 16) ** -0.5, 0.375, ((0, 4),))
    labels = with_ends(jax.random.randint(key_list[5], (MICRO, TOKENS), 0, LABELS), jax.random.fold_in(key_list[5], 1), 0, LABELS - 1).astype(jnp.int32)
    valid = draw_valid(jax.random.fold_in(key_list[7], 71), 0)
    return dict(inputs=inputs, adapter_down=adapter_down, adapter_up=adapter_up, gains=gains, head=head, labels=labels, valid=valid)


epsilon = 1e-05

def layer_forward(inbound, gain_row, down_weight, up_weight):
    values = inbound.astype(jnp.float32)
    squares = lax.optimization_barrier(jnp.sum(values * values, axis=1))
    inverse = lax.rsqrt(squares / D + epsilon)
    scaled = (values * gain_row).astype(jnp.bfloat16)
    projected = jnp.dot(scaled, down_weight, preferred_element_type=jnp.float32)
    hidden = jax.nn.silu(inverse[:, None] * projected).astype(jnp.bfloat16)
    outbound = (values + jnp.dot(hidden, up_weight, preferred_element_type=jnp.float32)).astype(jnp.bfloat16)
    return (outbound, projected, inverse)

def head_backward(final_state, head, label_row, valid_row):
    values = final_state.astype(jnp.float32)
    squares = lax.optimization_barrier(jnp.sum(values * values, axis=1))
    inverse = lax.rsqrt(squares / D + epsilon)
    logit_base = jnp.dot(final_state, head, preferred_element_type=jnp.float32)
    logits = inverse[:, None] * logit_base
    shifted = logits - lax.optimization_barrier(jnp.max(logits, axis=1, keepdims=True))
    expo_terms = jnp.exp(shifted)
    softmax_prob = expo_terms / lax.optimization_barrier(jnp.sum(expo_terms, axis=1, keepdims=True))
    classes = lax.broadcasted_iota(jnp.int32, logits.shape, 1)
    onehot = (classes == label_row[:, None]).astype(jnp.float32)
    cotangent = (softmax_prob - onehot) * valid_row[:, None].astype(jnp.float32)
    radial = lax.optimization_barrier(jnp.sum(cotangent * logit_base, axis=1))
    weighted = (inverse[:, None] * cotangent).astype(jnp.bfloat16)
    back_term = jnp.dot(weighted, head.T, preferred_element_type=jnp.float32)
    result = back_term - (inverse ** 3 / D * radial)[:, None] * values
    return result.astype(jnp.bfloat16)

def layer_backward(cotangent, inbound, projected, inverse, gain_row, down_weight, up_weight):
    hidden_grad = jnp.dot(cotangent, up_weight.T, preferred_element_type=jnp.float32)
    pre_act = inverse[:, None] * projected
    sigmoid_val = jax.nn.sigmoid(pre_act)
    act_grad = hidden_grad * sigmoid_val * (1.0 + pre_act * (1.0 - sigmoid_val))
    radial = lax.optimization_barrier(jnp.sum(act_grad * projected, axis=1))
    weighted = (inverse[:, None] * act_grad).astype(jnp.bfloat16)
    scaled_grad = jnp.dot(weighted, down_weight.T, preferred_element_type=jnp.float32)
    values = inbound.astype(jnp.float32)
    outbound = (cotangent.astype(jnp.float32) + gain_row * scaled_grad - (inverse ** 3 / D * radial)[:, None] * values).astype(jnp.bfloat16)
    scaled = (values * gain_row).astype(jnp.bfloat16)
    hidden = jax.nn.silu(pre_act).astype(jnp.bfloat16)
    down_grad = jnp.dot(scaled.T, weighted, preferred_element_type=jnp.float32)
    up_grad = jnp.dot(hidden.T, cotangent, preferred_element_type=jnp.float32)
    gain_grad = lax.optimization_barrier(jnp.sum(scaled_grad * values, axis=0))
    return (outbound, down_grad, up_grad, gain_grad)

def reference(inputs, adapter_down, adapter_up, gains, head, labels, valid):
    down_sums = [jnp.zeros((D, RANK), jnp.float32) for layer in range(SECTIONS)]
    up_sums = [jnp.zeros((RANK, D), jnp.float32) for layer in range(SECTIONS)]
    gain_sums = [jnp.zeros((D,), jnp.float32) for layer in range(SECTIONS)]
    for micro_index in range(MICRO):
        state = inputs[micro_index]
        saved = []
        for layer in range(SECTIONS):
            outbound, projected, inverse = layer_forward(state, gains[layer].astype(jnp.float32), adapter_down[layer], adapter_up[layer])
            saved.append((state, projected, inverse))
            state = outbound
        cotangent = head_backward(state, head, labels[micro_index], valid[micro_index])
        for layer in reversed(range(SECTIONS)):
            inbound, projected, inverse = saved[layer]
            cotangent, down_grad, up_grad, gain_grad = layer_backward(cotangent, inbound, projected, inverse, gains[layer].astype(jnp.float32), adapter_down[layer], adapter_up[layer])
            down_sums[layer] = down_sums[layer] + down_grad
            up_sums[layer] = up_sums[layer] + up_grad
            gain_sums[layer] = gain_sums[layer] + gain_grad
    total_count = jnp.sum(valid.astype(jnp.float32))
    return (jnp.stack(down_sums) / total_count, jnp.stack(up_sums) / total_count, jnp.stack(gain_sums) / total_count)
```

```python
import functools

import jax
import jax.numpy as jnp
from jax import lax
from jax.experimental import pallas as pl
from jax.experimental.pallas import tpu as pltpu
from jax.sharding import PartitionSpec as P

MESH = pl.DeviceIdType.MESH
epsilon = 1e-05
F32 = jnp.float32
BF16 = jnp.bfloat16


def mm(a, b):
    return jnp.dot(a, b, preferred_element_type=F32)


def mm_nt(a, b):
    return lax.dot_general(a, b, (((1,), (1,)), ((), ())), preferred_element_type=F32)


def mm_tn(a, b):
    return lax.dot_general(a, b, (((0,), (0,)), ((), ())), preferred_element_type=F32)


def split(v):
    high = v.astype(BF16)
    return high, (v - high.astype(F32)).astype(BF16)


def kernel(
    nt, nd, width,
    x_hbm, dn_hbm, up_hbm, gain_hbm, head_hbm, lab_hbm, val_hbm,
    out,
    x_ref, dn_ref, up_ref, gain_ref, head_ref, lab_ref, val_ref,
    odn, oup, ogain, stok, rtok, sgram, rgram, pgram, gall, sres, res, sdp, rdp, rin, relay, psum, rcross, sgn, rgn,
    load, sib_s, sib_r, tok_s, tok_r, gr_s, gr_r, ga_s, ga_r, re_s, re_r, fw_s, fw_r, dp_s, dp_r, rel_s, rel_r, cr_s, cr_r,
):
    s, d, t = lax.axis_index("section"), lax.axis_index("dp"), lax.axis_index("tensor")
    first = s == 0
    tokens, feats = x_ref.shape
    rank = dn_ref.shape[1]
    half = tokens // 2
    own = half // nt
    rows = rank // nt
    part = rank // nd
    wire = stok.dtype

    def peer(k, other):
        return (1 - s if other else s, d, lax.rem(t + k, nt))

    group = [(k, o) for k in range(nt) for o in (0, 1) if (k, o) != (0, 0)]

    loads = [
        pltpu.make_async_copy(a, b, load.at[i])
        for i, (a, b) in enumerate((
            (up_hbm, up_ref), (head_hbm, head_ref), (x_hbm, x_ref), (gain_hbm, gain_ref),
            (dn_hbm, dn_ref), (lab_hbm, lab_ref), (val_hbm, val_ref),
        ))
    ]
    for c in loads:
        c.start()

    barrier = pltpu.get_barrier_semaphore()
    for k, o in group:
        pl.semaphore_signal(barrier, inc=1, device_id=peer(k, o), device_id_type=MESH)
    for k in range(1, nd):
        pl.semaphore_signal(barrier, inc=1, device_id=(s, lax.rem(d + k, nd), t), device_id_type=MESH)

    def send(src, dst, ss, rs, to):
        copy = pltpu.make_async_remote_copy(
            src_ref=src, dst_ref=dst, send_sem=ss, recv_sem=rs, device_id=to, device_id_type=MESH
        )
        copy.start()
        return copy

    def put_gram(j, g):
        g = g.astype(wire)
        for i in range(nt):
            sgram[i, j] = g[i * rows : (i + 1) * rows]

    loads[0].wait()
    up = up_ref[...]
    put_gram(0, mm_nt(up, up))
    loads[1].wait()
    head = head_ref[...]
    put_gram(1, mm(up, head))
    for c in loads[2:]:
        c.wait()
    gain = gain_ref[...].astype(F32)
    xb = x_ref[...]
    xf = xb.astype(F32)
    xup = mm_nt(xb, up).astype(wire)
    proj = mm((xf * gain).astype(BF16), dn_ref[...]).astype(wire)
    for b in range(2):
        for i in range(nt):
            at = b * half + i * own
            stok[b, i, 0] = proj[at : at + own]
            stok[b, i, 1] = xup[at : at + own]

    pl.semaphore_wait(barrier, len(group) + nd - 1)

    sib = [
        send(a, b, sib_s.at[i], sib_r.at[i], peer(0, 1))
        for i, (a, b) in enumerate(((up_ref, oup), (dn_ref, odn), (gain_ref, ogain)))
    ]
    started = list(sib)
    spans = (pl.ds(0, 2), pl.ds(2, 1))

    def scatter_gram(j):
        copies = [
            send(
                sgram.at[lax.rem(t + k, nt), spans[j]], rgram.at[k, spans[j]],
                gr_s.at[j, k], gr_r.at[j, k], peer(k, 0),
            )
            for k in range(1, nt)
        ]
        started.extend(copies)
        return copies

    def gather_gram(j, copies):
        total = sgram[t, spans[j]].astype(F32)
        for k in range(1, nt):
            copies[k - 1].wait_recv()
            total = total + rgram[k, spans[j]].astype(F32)
        total = total.astype(wire)
        pgram[spans[j]] = total
        gall[s, t, spans[j]] = total
        out_copies = [
            send(
                pgram.at[spans[j]], gall.at[s, t, spans[j]],
                ga_s.at[j, o, k], ga_r.at[j, o, k], peer(k, o),
            )
            for k, o in group
        ]
        started.extend(out_copies)
        return out_copies

    ab_copies = scatter_gram(0)
    tok_copies = {}
    for k in range(nt):
        to = lax.rem(t + k, nt)
        tok_copies[k, 1] = send(
            stok.at[1 - s, to, pl.ds(0, 2)], rtok.at[1, k, pl.ds(0, 2)],
            tok_s.at[1, k], tok_r.at[1, k], peer(k, 1),
        )
    xm = x_ref[pl.ds(pl.multiple_of(s * half, half), half), :]
    xmf = xm.astype(F32)
    xhead = mm(xm, head)
    squares = jnp.broadcast_to(jnp.sum(xmf * xmf, axis=1, keepdims=True), (half, rank))
    hh, hl = split(xhead)
    qh, ql = split(squares)
    lane_h = lax.broadcasted_iota(jnp.int32, (half, rank), 1)
    q = jnp.where(lane_h < rank // 2, qh.astype(F32), ql.astype(F32)).astype(wire)
    hh, hl = hh.astype(wire), hl.astype(wire)
    for i in range(nt):
        stok[s, i, 2] = hh[i * own : (i + 1) * own]
        stok[s, i, 3] = hl[i * own : (i + 1) * own]
        stok[s, i, 4] = q[i * own : (i + 1) * own]

    sib[0].wait_recv()
    gram_c = mm_nt(up, oup[...])
    gram_d = mm((oup[...].astype(F32) * gain).astype(BF16), dn_ref[...])
    put_gram(2, jnp.where(first, gram_c, gram_d))
    c_copies = scatter_gram(1)
    for k in range(1, nt):
        to = lax.rem(t + k, nt)
        tok_copies[k, 0] = send(
            stok.at[s, to], rtok.at[0, k], tok_s.at[0, k], tok_r.at[0, k], peer(k, 0)
        )
    started += list(tok_copies.values())
    all_copies = gather_gram(0, ab_copies)
    all_copies = all_copies + gather_gram(1, c_copies)

    lab = jnp.where(first, lab_ref[0:1, :], lab_ref[1:2, :])
    val = jnp.where(first, val_ref[0:1, :], val_ref[1:2, :]).astype(F32)
    labels_n = head.shape[1]
    hot_t = jnp.where(lax.broadcasted_iota(jnp.int32, (labels_n, half), 0) == lab, val, 0.0).astype(BF16)
    val_t = jnp.broadcast_to(val, (labels_n, half)).astype(BF16)
    pick = (
        lax.broadcasted_iota(jnp.int32, (own, half), 0) + t * own
        == lax.broadcasted_iota(jnp.int32, (own, half), 1)
    ).astype(F32).astype(BF16)
    onehot = mm_nt(pick, hot_t)
    validity = mm_nt(pick, val_t)
    count = jnp.sum(val_ref[...].astype(F32))

    mine = stok[s, t].astype(F32)
    for k in range(1, nt):
        tok_copies[k, 0].wait_recv()
        mine = mine + rtok[0, k].astype(F32)
    tok_copies[0, 1].wait_recv()
    theirs = rtok[1, 0, 0:2].astype(F32)
    for k in range(1, nt):
        tok_copies[k, 1].wait_recv()
        theirs = theirs + rtok[1, k, 0:2].astype(F32)
    p0 = jnp.where(first, mine[0], theirs[0])
    p1 = jnp.where(first, theirs[0], mine[0])
    v0 = jnp.where(first, mine[1], theirs[1])
    v1 = jnp.where(first, theirs[1], mine[1])
    xh = mine[2] + mine[3]
    sq0 = mine[4][:, 0:1] + mine[4][:, rank // 2 : rank // 2 + 1]

    for c in all_copies:
        c.wait_recv()

    def gram(a, j):
        return gall[a, :, j].reshape(rank, rank).astype(BF16)

    a0, b0, c0 = gram(0, 0), gram(0, 1), gram(0, 2)
    a1, b1, d1 = gram(1, 0), gram(1, 1), gram(1, 2)

    def rowsum(v):
        return jnp.sum(v, axis=1, keepdims=True)

    inv0 = lax.rsqrt(sq0 / width + epsilon)
    pre0 = inv0 * p0
    sig0 = jax.nn.sigmoid(pre0)
    h0 = (pre0 * sig0).astype(BF16)
    h0f = h0.astype(F32)
    h0a = mm(h0, a0)
    p1 = p1 + mm(h0, d1)
    s1u0 = v0 + h0a
    s1u1 = v1 + mm(h0, c0)
    base = xh + mm(h0, b0)
    sq1 = sq0 + rowsum(h0f * (v0 + s1u0))
    inv1 = lax.rsqrt(sq1 / width + epsilon)
    pre1 = inv1 * p1
    sig1 = jax.nn.sigmoid(pre1)
    h1 = (pre1 * sig1).astype(BF16)
    h1f = h1.astype(F32)
    yu1 = s1u1 + mm(h1, a1)
    yu0 = s1u0 + mm_nt(h1, c0)
    base = base + mm(h1, b1)
    sq2 = sq1 + rowsum(h1f * (s1u1 + yu1))
    inv2 = lax.rsqrt(sq2 / width + epsilon)
    logits = inv2 * base
    expo = jnp.exp(logits - jnp.max(logits, axis=1, keepdims=True))
    cot = expo / rowsum(expo) * validity - onehot
    radial = rowsum(cot * base)
    wh = (inv2 * cot).astype(BF16)
    ch = inv2 * inv2 * inv2 / width * radial
    hg1 = mm_nt(wh, b1) - ch * yu1
    act1 = hg1 * sig1 * (1.0 + pre1 * (1.0 - sig1))
    w1 = (inv1 * act1).astype(BF16)
    c1 = inv1 * inv1 * inv1 / width * rowsum(act1 * p1)
    hg0 = mm_nt(wh, b0) - ch * yu0 + mm_nt(w1, d1) - c1 * s1u0
    act0 = hg0 * sig0 * (1.0 + pre0 * (1.0 - sig0))
    w0 = (inv0 * act0).astype(BF16)

    ch_h, ch_l = split(ch)
    c1_h, c1_l = split(c1)
    lane = lax.broadcasted_iota(jnp.int32, (own, rank), 1)
    q4 = rank // 4
    coef = jnp.where(
        lane < q4, ch_h.astype(F32),
        jnp.where(lane < 2 * q4, ch_l.astype(F32), jnp.where(lane < 3 * q4, c1_h.astype(F32), c1_l.astype(F32))),
    )
    for j, v in enumerate((h0, h1, w0, w1, wh, coef)):
        v = v.astype(wire)
        sres[j] = v
        res[s, t, j] = v
    res_copies = {
        k: send(sres, res.at[s, t], re_s.at[k], re_r.at[k], peer(k, 0 if k else 1)) for k in range(nt)
    }
    forwards = []
    for k in range(1, nt):
        res_copies[k].wait_recv()
        at = lax.rem(t + nt - k, nt)
        forwards.append(send(res.at[s, at], res.at[s, at], fw_s.at[k], fw_r.at[k], peer(0, 1)))
    started += list(res_copies.values()) + forwards
    sib[1].wait_recv()
    sib[2].wait_recv()
    res_copies[0].wait_recv()
    for c in forwards:
        c.wait_recv()

    def got(j):
        return res[:, :, j].reshape(tokens, res.shape[-1])

    def piece(j, full):
        full = full.astype(BF16)
        for i in range(nd):
            sdp[i, j] = full[i * part : (i + 1) * part]

    hl = nd // 2
    side = d // hl
    local_d = lax.rem(d, hl)
    far = (1 - side) * hl
    odd = lax.rem(d, 2)
    outer = odd == side

    def remote(src, dst, ss, rs, to):
        return pltpu.make_async_remote_copy(
            src_ref=src, dst_ref=dst, send_sem=ss, recv_sem=rs, device_id=(s, to, t), device_id_type=MESH
        )

    def up_copy(k):
        to = lax.rem(d + k, nd)
        return remote(sdp.at[to, 1], rdp.at[k], dp_s.at[0, k], dp_r.at[0, k], to)

    def near_copy(k):
        to = side * hl + lax.rem(local_d + k, hl)
        return remote(sdp.at[to, 0], rin.at[k], dp_s.at[1, k], dp_r.at[1, k], to)

    def relay_copy():
        return remote(sdp.at[pl.ds(far, hl), 0], relay, rel_s, rel_r, d + 1 - 2 * odd)

    def cross_copy(i):
        m = local_d // 2
        return remote(psum.at[i], rcross.at[m], cr_s.at[i], cr_r.at[m], far + i)

    def cross_wait(m):
        return remote(psum.at[0], rcross.at[m], cr_s.at[0], cr_r.at[m], far)

    def finish(state, own_w, own_h, cotangent):
        scaled = (state * gain).astype(BF16)
        piece(0, mm_tn(own_w, scaled))

        @pl.when(outer)
        def _():
            relay_copy().start()

        gain_row = jnp.sum(mm_nt(own_w, dn_ref[...]) * state, axis=0, keepdims=True)
        sgn[0:1, :] = gain_row
        sgn[1:2, :] = jnp.full((1, feats), count, F32)
        piece(1, mm_tn(own_h, cotangent().astype(BF16)))
        for k in sorted(range(1, nd), key=lambda k: abs(k - hl)):
            up_copy(k).start()
        for k in range(1, hl):
            near_copy(k).start()

    h0g, h1g, w1g, whg = (got(j).astype(BF16) for j in (0, 1, 3, 4))
    cg = got(5).astype(F32)
    chg = cg[:, 0:1] + cg[:, q4 : q4 + 1]
    c1g = cg[:, 2 * q4 : 2 * q4 + 1] + cg[:, 3 * q4 : 3 * q4 + 1]

    @pl.when(s == 0)
    def _():
        def cotangent():
            s1 = xf + mm(h0g, up)
            y = s1 + mm(h1g, oup[...])
            g2 = mm_nt(whg, head) - chg * y
            return g2 + ogain[...].astype(F32) * mm_nt(w1g, odn[...]) - c1g * s1

        finish(xf, got(2).astype(BF16), h0g, cotangent)

    @pl.when(s != 0)
    def _():
        s1 = xf + mm(h0g, oup[...])

        def cotangent():
            y = s1 + mm(h1g, up)
            return mm_nt(whg, head) - chg * y

        finish(s1, w1g, h1g, cotangent)

    small_copies = [
        send(sgn, rgn.at[k], dp_s.at[2, k], dp_r.at[2, k], (s, lax.rem(d + k, nd), t)) for k in range(1, nd)
    ]
    started += small_copies

    @pl.when(jnp.logical_not(outer))
    def _():
        relay_copy().wait_recv()
        psum[...] = (sdp[pl.ds(far, hl), 0].astype(F32) + relay[...].astype(F32)).astype(BF16)
        for i in range(hl):
            cross_copy(i).start()

    small = sgn[...]
    for k in range(1, nd):
        small_copies[k - 1].wait_recv()
        small = small + rgn[k]
    out[2 * part : 2 * part + 2, :] = small
    sums = sdp[d, 1].astype(F32)
    for k in range(1, nd):
        up_copy(k).wait_recv()
        sums = sums + rdp[k].astype(F32)
    out[part : 2 * part, :] = sums
    sums = sdp[d, 0].astype(F32)
    for k in range(1, hl):
        near_copy(k).wait_recv()
        sums = sums + rin[k].astype(F32)
    for m in range(nd // 4):
        cross_wait(m).wait_recv()
        sums = sums + rcross[m].astype(F32)
    out[0:part, :] = sums

    @pl.when(outer)
    def _():
        relay_copy().wait_send()

    @pl.when(jnp.logical_not(outer))
    def _():
        for i in range(hl):
            cross_copy(i).wait_send()

    for k in range(1, nd):
        up_copy(k).wait_send()
    for k in range(1, hl):
        near_copy(k).wait_send()
    for c in started:
        c.wait_send()


def scale_kernel(part, sums, down_out, up_out, gain_out):
    scale = 1.0 / sums[2 * part + 1 : 2 * part + 2, :]
    down_out[...] = sums[0:part, :] * scale
    up_out[...] = sums[part : 2 * part, :] * scale
    gain_out[...] = sums[2 * part : 2 * part + 1, :] * scale


def solution(mesh):
    nt, nd, ns = mesh.shape["tensor"], mesh.shape["dp"], mesh.shape["section"]
    assert ns == 2 and nd % 4 == 0

    def local(inputs, down, up, gains, head, labels, valid):
        micro, per, feats = inputs.shape
        assert micro == ns
        tokens = micro * per
        rank = down.shape[2]
        own, rows, part = tokens // ns // nt, rank // nt, rank // nd
        wire = BF16 if own % 16 == 0 and rows % 16 == 0 else F32
        vmem = pl.BlockSpec(memory_space=pltpu.VMEM)
        dma = pltpu.SemaphoreType.DMA
        anyspace = pl.BlockSpec(memory_space=pl.ANY)
        sums = pl.pallas_call(
            functools.partial(kernel, nt, nd, feats * nt),
            out_shape=pltpu.VMEM((2 * part + 8, feats), F32),
            in_specs=[anyspace] * 7,
            out_specs=vmem,
            scratch_shapes=[
                pltpu.VMEM((tokens, feats), BF16),
                pltpu.VMEM((feats, rank), BF16),
                pltpu.VMEM((rank, feats), BF16),
                pltpu.VMEM((1, feats), BF16),
                pltpu.VMEM((feats, head.shape[1]), BF16),
                pltpu.VMEM((micro, per), jnp.int32),
                pltpu.VMEM((micro, per), jnp.int32),
                pltpu.VMEM((feats, rank), BF16),
                pltpu.VMEM((rank, feats), BF16),
                pltpu.VMEM((1, feats), BF16),
                pltpu.VMEM((2, nt, 5, own, rank), wire),
                pltpu.VMEM((2, nt, 5, own, rank), wire),
                pltpu.VMEM((nt, 3, rows, rank), wire),
                pltpu.VMEM((nt, 3, rows, rank), wire),
                pltpu.VMEM((3, rows, rank), wire),
                pltpu.VMEM((2, nt, 3, rows, rank), wire),
                pltpu.VMEM((6, own, rank), wire),
                pltpu.VMEM((2, nt, 6, own, rank), wire),
                pltpu.VMEM((nd, 2, part, feats), BF16),
                pltpu.VMEM((nd, part, feats), BF16),
                pltpu.VMEM((nd // 2, part, feats), BF16),
                pltpu.VMEM((nd // 2, part, feats), BF16),
                pltpu.VMEM((nd // 2, part, feats), BF16),
                pltpu.VMEM((nd // 4, part, feats), BF16),
                pltpu.VMEM((2, feats), F32),
                pltpu.VMEM((nd, 2, feats), F32),
                dma((7,)),
                dma((3,)), dma((3,)),
                dma((2, nt)), dma((2, nt)),
                dma((2, nt)), dma((2, nt)),
                dma((2, 2, nt)), dma((2, 2, nt)),
                dma((nt,)), dma((nt,)),
                dma((nt,)), dma((nt,)),
                dma((3, nd)), dma((3, nd)),
                dma, dma,
                dma((nd // 2,)), dma((nd // 4,)),
            ],
            compiler_params=pltpu.CompilerParams(collective_id=0, has_side_effects=True),
        )(inputs.reshape(tokens, feats), down[0], up[0], gains, head, labels, valid)
        down_t, up_g, gain_g = pl.pallas_call(
            functools.partial(scale_kernel, part),
            out_shape=(
                jax.ShapeDtypeStruct((part, feats), F32),
                jax.ShapeDtypeStruct((part, feats), F32),
                jax.ShapeDtypeStruct((1, feats), F32),
            ),
            in_specs=[vmem],
            out_specs=(vmem,) * 3,
        )(pltpu.with_memory_space_constraint(sums, pltpu.VMEM))
        return down_t.T[None], up_g[None], gain_g

    return jax.shard_map(
        local,
        mesh=mesh,
        in_specs=(
            P(None, "dp", "tensor"),
            P("section", "tensor", None),
            P("section", None, "tensor"),
            P("section", "tensor"),
            P("tensor", None),
            P(None, "dp"),
            P(None, "dp"),
        ),
        out_specs=(
            P("section", "tensor", "dp"),
            P("section", "dp", "tensor"),
            P("section", "tensor"),
        ),
        check_vma=False,
    )
```

```python
import functools

import jax
import jax.numpy as jnp
from jax import lax
from jax.experimental import pallas as pl
from jax.experimental.pallas import tpu as pltpu
from jax.sharding import PartitionSpec as P

MESH = pl.DeviceIdType.MESH
epsilon = 1e-05
F32 = jnp.float32
BF16 = jnp.bfloat16


def mm(a, b):
    return jnp.dot(a, b, preferred_element_type=F32)


def mm_nt(a, b):
    return lax.dot_general(a, b, (((1,), (1,)), ((), ())), preferred_element_type=F32)


def mm_tn(a, b):
    return lax.dot_general(a, b, (((0,), (0,)), ((), ())), preferred_element_type=F32)


def split(v):
    high = v.astype(BF16)
    return high, (v - high.astype(F32)).astype(BF16)


def kernel(
    nt, nd, width,
    x_hbm, dn_hbm, up_hbm, gain_hbm, head_hbm, lab_hbm, val_hbm,
    out,
    x_ref, dn_ref, up_ref, gain_ref, head_ref, lab_ref, val_ref,
    odn, oup, ogain, stok, rtok, ssq, rsq, sgram, rgram, pgram, gall, sres, res,
    sdp, rnear, rfar, relay, psum, rcross, sgn, rsm, spr, rgn,
    load, sib_s, sib_r, tok_s, tok_r, sq_s, sq_r, gr_s, gr_r, gq_s, gq_r, ga_s, ga_r, gf_s, gf_r, gc_s, gc_r,
    re_s, re_r, fw_s, fw_r, dp_s, dp_r, far_s, far_r, rel_s, rel_r, cr_s, cr_r, sm_s, sm_r, su_s, su_r,
):
    s, d, t = lax.axis_index("section"), lax.axis_index("dp"), lax.axis_index("tensor")
    first = s == 0
    tokens, feats = x_ref.shape
    rank = dn_ref.shape[1]
    half = tokens // 2
    own = half // nt
    rows = rank // nt
    part = rank // nd
    wire = stok.dtype

    hl = nd // 2
    quarter = hl // 2
    side = d // hl
    local_d = lax.rem(d, hl)
    far = (1 - side) * hl
    odd = lax.rem(d, 2)
    outer = odd == side
    deep = local_d // quarter == side
    tip = jnp.logical_and(outer, deep)
    partner = d + 1 - 2 * odd

    def ahead(k):
        return lax.rem(t + k, nt)

    def behind(k):
        return lax.rem(t + nt - k, nt)

    loads = [
        pltpu.make_async_copy(a, b, load.at[i])
        for i, (a, b) in enumerate((
            (up_hbm, up_ref), (head_hbm, head_ref), (x_hbm, x_ref), (gain_hbm, gain_ref),
            (dn_hbm, dn_ref), (lab_hbm, lab_ref), (val_hbm, val_ref),
        ))
    ]
    for c in loads:
        c.start()

    barrier = pltpu.get_barrier_semaphore()
    for k in range(1, nd):
        to = lax.rem(d + k, nd)

        @pl.when(jnp.logical_not(jnp.logical_and(tip, to == nd - 1 - d)))
        def _():
            pl.semaphore_signal(barrier, inc=1, device_id=(s, to, t), device_id_type=MESH)

    group = [(k, o) for k in range(nt) for o in (0, 1) if (k, o) != (0, 0)]
    for k, o in group:
        pl.semaphore_signal(barrier, inc=1, device_id=(1 - s if o else s, d, ahead(k)), device_id_type=MESH)

    def copy(src, dst, ss, rs, section, column):
        return pltpu.make_async_remote_copy(
            src_ref=src, dst_ref=dst, send_sem=ss, recv_sem=rs, device_id=(section, d, column), device_id_type=MESH
        )

    def put_gram(j, g):
        g = g.astype(wire)
        for i in range(nt):
            sgram[i, j] = g[i * rows : (i + 1) * rows]

    loads[0].wait()
    up = up_ref[...]
    put_gram(0, mm_nt(up, up))
    loads[1].wait()
    head = head_ref[...]
    put_gram(1, mm(up, head))

    pl.semaphore_wait(barrier, len(group) + nd - 1 - tip.astype(jnp.int32))

    def sib(i):
        a, b = ((up_ref, oup), (dn_ref, odn), (gain_ref, ogain))[i]
        return copy(a, b, sib_s.at[i], sib_r.at[i], 1 - s, t)

    def ab_scatter(k, sender):
        return copy(
            sgram.at[ahead(k), pl.ds(0, 2)], rgram.at[sender, k, pl.ds(0, 2)], gr_s.at[k], gr_r.at[sender, k], 1, ahead(k)
        )

    def cd_scatter(k):
        return copy(sgram.at[ahead(k), pl.ds(2, 2)], rgram.at[1, k, pl.ds(2, 2)], gq_s.at[k], gq_r.at[k], 1, ahead(k))

    def tok_cross(k):
        block = pl.ds(0, 2)
        return copy(
            stok.at[1 - s, ahead(k), block], rtok.at[1, k, block], tok_s.at[1, k], tok_r.at[1, k], 1 - s, ahead(k)
        )

    def tok_own(k):
        return copy(stok.at[s, ahead(k)], rtok.at[0, k], tok_s.at[0, k], tok_r.at[0, k], s, ahead(k))

    def sq_own(k):
        return copy(ssq, rsq.at[k], sq_s.at[k], sq_r.at[k], s, ahead(k))

    def ab_gather(k, section):
        block = pl.ds(0, 4)
        return copy(pgram.at[block], gall.at[t, block], ga_s.at[k], ga_r.at[k], section, ahead(k))

    def ab_forward(k):
        block = gall.at[behind(k), pl.ds(0, 4)]
        return copy(block, block, gf_s.at[k], gf_r.at[k], 0, t)

    def cd_gather(k, section):
        block = pl.ds(4, 2)
        return copy(pgram.at[block], gall.at[t, block], gc_s.at[section, k], gc_r.at[k], section, ahead(k))

    sib(0).start()
    for k in range(1, nt):
        ab_scatter(k, s).start()

    @pl.when(first)
    def _():
        ab_scatter(0, 0).start()

    for c in loads[2:]:
        c.wait()
    gain = gain_ref[...].astype(F32)
    xb = x_ref[...]
    xf = xb.astype(F32)
    xup = mm_nt(xb, up).astype(wire)
    proj = mm((xf * gain).astype(BF16), dn_ref[...]).astype(wire)
    for b in range(2):
        for i in range(nt):
            at = b * half + i * own
            stok[b, i, 0] = proj[at : at + own]
            stok[b, i, 1] = xup[at : at + own]
    for k in range(nt):
        tok_cross(k).start()

    xm = x_ref[pl.ds(pl.multiple_of(s * half, half), half), :]
    xmf = xm.astype(F32)
    xhead = mm(xm, head).astype(wire)
    for i in range(nt):
        stok[s, i, 2] = xhead[i * own : (i + 1) * own]
    ones = jnp.ones((8, feats), BF16)
    square_h, square_l = split(xmf * xmf)
    row_h, row_l = split(mm_nt(ones, square_h) + mm_nt(ones, square_l))
    ssq[0:8] = row_h.astype(wire)
    ssq[8:16] = row_l.astype(wire)

    @pl.when(s != 0)
    def _():
        sib(0).wait_recv()
        other = oup[...]
        put_gram(2, mm_nt(other, up))
        put_gram(3, mm((other.astype(F32) * gain).astype(BF16), dn_ref[...]))
        for k in range(1, nt):
            cd_scatter(k).start()

    for k in range(1, nt):
        tok_own(k).start()
        sq_own(k).start()

    @pl.when(s != 0)
    def _():
        sib(1).start()
        sib(2).start()
        ab_scatter(0, 0).wait_recv()
        mine0 = rgram[0, 0, 0:2].astype(F32)
        mine1 = sgram[t, 0:2].astype(F32)
        for k in range(1, nt):
            ab_scatter(k, 1).wait_recv()
            mine1 = mine1 + rgram[1, k, 0:2].astype(F32)
        for k in range(1, nt):
            ab_scatter(k, 0).wait_recv()
            mine0 = mine0 + rgram[0, k, 0:2].astype(F32)
        for j, v in ((0, mine0.astype(wire)), (2, mine1.astype(wire))):
            pgram[j : j + 2] = v
            gall[t, j : j + 2] = v
        for k in range(1, nt):
            ab_gather(k, 1).start()
        ab_gather(0, 0).start()
        both = sgram[t, 2:4].astype(F32)
        for k in range(1, nt):
            cd_scatter(k).wait_recv()
            both = both + rgram[1, k, 2:4].astype(F32)
        both = both.astype(wire)
        pgram[4:6] = both
        gall[t, 4:6] = both
        for k in range(1, nt):
            cd_gather(k, 1).start()
        for k in range(nt):
            cd_gather(k, 0).start()

    lab = jnp.where(first, lab_ref[0:1, :], lab_ref[1:2, :])
    val = jnp.where(first, val_ref[0:1, :], val_ref[1:2, :]).astype(F32)
    labels_n = head.shape[1]
    hot_t = jnp.where(lax.broadcasted_iota(jnp.int32, (labels_n, half), 0) == lab, val, 0.0).astype(BF16)
    val_t = jnp.broadcast_to(val, (labels_n, half)).astype(BF16)
    chosen = (
        lax.broadcasted_iota(jnp.int32, (own, half), 0) + t * own
        == lax.broadcasted_iota(jnp.int32, (own, half), 1)
    )
    pick = chosen.astype(F32).astype(BF16)
    onehot = mm_nt(pick, hot_t)
    validity = mm_nt(pick, val_t)
    count = jnp.sum(val_ref[...].astype(F32))

    mine = stok[s, t].astype(F32)
    for k in range(1, nt):
        tok_own(k).wait_recv()
        mine = mine + rtok[0, k].astype(F32)
    tok_cross(0).wait_recv()
    theirs = rtok[1, 0, 0:2].astype(F32)
    for k in range(1, nt):
        tok_cross(k).wait_recv()
        theirs = theirs + rtok[1, k, 0:2].astype(F32)
    p0 = jnp.where(first, mine[0], theirs[0])
    p1 = jnp.where(first, theirs[0], mine[0])
    v0 = jnp.where(first, mine[1], theirs[1])
    v1 = jnp.where(first, theirs[1], mine[1])
    xh = mine[2]
    sq = ssq[...].astype(F32)
    for k in range(1, nt):
        sq_own(k).wait_recv()
        sq = sq + rsq[k].astype(F32)

    def rowsum(v):
        return jnp.sum(v, axis=1, keepdims=True)

    sq0 = rowsum(jnp.where(chosen, sq[0:1] + sq[8:9], 0.0))
    inv0 = lax.rsqrt(sq0 / width + epsilon)
    pre0 = inv0 * p0
    sig0 = jax.nn.sigmoid(pre0)
    h0 = (pre0 * sig0).astype(BF16)
    h0f = h0.astype(F32)

    @pl.when(s != 0)
    def _():
        for k in range(1, nt):
            ab_gather(k, 1).wait_recv()
            ab_forward(k).start()
        for k in range(1, nt):
            cd_gather(k, 1).wait_recv()

    @pl.when(first)
    def _():
        ab_gather(0, 0).wait_recv()
        for k in range(1, nt):
            ab_forward(k).wait_recv()
        for k in range(nt):
            cd_gather(k, 0).wait_recv()

    def gram(j):
        return gall[:, j].reshape(rank, rank).astype(BF16)

    a0, b0, a1, b1, c0, d1 = (gram(j) for j in range(6))

    parts = ((0, 2), (2, 4))

    def keep(j, v):
        v = v.astype(wire)
        sres[j] = v
        res[s, t, j] = v

    def shared(m, k, sender):
        at, size = parts[m]
        span = pl.ds(at, size)
        return copy(
            sres.at[span], res.at[sender, t, span], re_s.at[m, k], re_r.at[m, sender, k], 1 if k else 1 - sender, ahead(k)
        )

    def onward(m, k, sender):
        at, size = parts[m]
        block = res.at[sender, behind(k), pl.ds(at, size)]
        return copy(block, block, fw_s.at[m, sender, k], fw_r.at[m, sender, k], 0, t)

    def share(m):
        for k in list(range(1, nt)) + [0]:
            shared(m, k, s).start()

    h0a = mm(h0, a0)
    p1 = p1 + mm(h0, d1)
    s1u0 = v0 + h0a
    s1u1 = v1 + mm(h0, c0)
    base = xh + mm(h0, b0)
    sq1 = sq0 + rowsum(h0f * (v0 + s1u0))
    inv1 = lax.rsqrt(sq1 / width + epsilon)
    pre1 = inv1 * p1
    sig1 = jax.nn.sigmoid(pre1)
    h1 = (pre1 * sig1).astype(BF16)
    h1f = h1.astype(F32)
    keep(0, h0)
    keep(1, h1)
    share(0)
    yu1 = s1u1 + mm(h1, a1)
    yu0 = s1u0 + mm_nt(h1, c0)
    base = base + mm(h1, b1)
    sq2 = sq1 + rowsum(h1f * (s1u1 + yu1))
    inv2 = lax.rsqrt(sq2 / width + epsilon)
    logits = inv2 * base
    expo = jnp.exp(logits - jnp.max(logits, axis=1, keepdims=True))
    cot = expo / rowsum(expo) * validity - onehot
    radial = rowsum(cot * base)
    wh = (inv2 * cot).astype(BF16)
    keep(2, wh)
    ch = inv2 * inv2 * inv2 / width * radial
    hg1 = mm_nt(wh, b1) - ch * yu1
    act1 = hg1 * sig1 * (1.0 + pre1 * (1.0 - sig1))
    w1 = (inv1 * act1).astype(BF16)
    c1 = inv1 * inv1 * inv1 / width * rowsum(act1 * p1)
    ch_h, ch_l = split(ch)
    c1_h, c1_l = split(c1)
    lane = lax.broadcasted_iota(jnp.int32, (own, rank), 1)
    q4 = rank // 4
    keep(3, w1)
    keep(4, jnp.where(
        lane < q4, ch_h.astype(F32),
        jnp.where(lane < 2 * q4, ch_l.astype(F32), jnp.where(lane < 3 * q4, c1_h.astype(F32), c1_l.astype(F32))),
    ))
    hg0 = mm_nt(wh, b0) - ch * yu0 + mm_nt(w1, d1) - c1 * s1u0
    act0 = hg0 * sig0 * (1.0 + pre0 * (1.0 - sig0))
    w0 = (inv0 * act0).astype(BF16)
    keep(5, w0)
    share(1)

    def got(j):
        return res[:, :, j].reshape(tokens, res.shape[-1])

    def piece(j, full):
        full = full.astype(BF16)
        for i in range(nd):
            sdp[i, j] = full[i * part : (i + 1) * part]

    near_far = far + side * quarter
    deep_far = far + (1 - side) * quarter

    def remote(src, dst, ss, rs, to):
        return pltpu.make_async_remote_copy(
            src_ref=src, dst_ref=dst, send_sem=ss, recv_sem=rs, device_id=(s, to, t), device_id_type=MESH
        )

    def near_copy(k, j):
        to = side * hl + lax.rem(local_d + k, hl)
        return remote(sdp.at[to, j], rnear.at[j, k], dp_s.at[j, k], dp_r.at[j, k], to)

    def up_copy(i):
        return remote(sdp.at[near_far + i, 1], rfar.at[local_d], far_s.at[i], far_r.at[local_d], near_far + i)

    def up_wait(m):
        return remote(sdp.at[far, 1], rfar.at[m], far_s.at[0], far_r.at[m], far)

    def relay_copy(g):
        block = pl.ds(near_far if g == 2 else deep_far, quarter)
        return remote(sdp.at[block, 1 if g == 1 else 0], relay.at[g], rel_s.at[g], rel_r.at[g], partner)

    def cross_copy(g, i):
        m = local_d // 2
        to = (near_far if g == 2 else deep_far) + i
        return remote(psum.at[g, i], rcross.at[1 if g == 1 else 0, m], cr_s.at[g, i], cr_r.at[1 if g == 1 else 0, m], to)

    def cross_wait(j, m):
        return remote(psum.at[0, 0], rcross.at[j, m], cr_s.at[0, 0], cr_r.at[j, m], near_far)

    def small_copy(k):
        return remote(spr, rgn.at[d // 2], sm_s.at[k], sm_r.at[d // 2], lax.rem(d + k, nd))

    def small_wait(p):
        return remote(spr, rgn.at[p], sm_s.at[1], sm_r.at[p], partner)

    def small_first():
        return remote(sgn, rsm, su_s, su_r, partner)

    def tail(sec):
        u0, u1 = (oup, up_ref) if sec else (up_ref, oup)
        senders = [(k, b) for k in range(1, nt) for b in (1, 0)]

        def collect(m):
            if sec:
                for k, b in senders:
                    shared(m, k, b).wait_recv()
                    onward(m, k, b).start()
                shared(m, 0, 0).wait_recv()
            else:
                shared(m, 0, 1).wait_recv()
                for k, b in senders:
                    onward(m, k, b).wait_recv()

        if sec == 0:
            for i in range(3):
                sib(i).wait_recv()
        collect(0)
        h0g, h1g = got(0).astype(BF16), got(1).astype(BF16)
        s1 = xf + mm(h0g, u0[...])
        y = s1 + mm(h1g, u1[...])
        collect(1)
        w1g = got(3).astype(BF16)
        state, own_w = (s1, w1g) if sec else (xf, got(5).astype(BF16))
        piece(0, mm_tn(own_w, (state * gain).astype(BF16)))

        @pl.when(outer)
        def _():
            relay_copy(0).start()

        @pl.when(jnp.logical_not(outer))
        def _():
            for k in range(1, hl):
                near_copy(k, 0).start()

        cg = got(4).astype(F32)
        chg = cg[:, 0:1] + cg[:, q4 : q4 + 1]
        g = mm_nt(got(2).astype(BF16), head_ref[...]) - chg * y
        if sec == 0:
            c1g = cg[:, 2 * q4 : 2 * q4 + 1] + cg[:, 3 * q4 : 3 * q4 + 1]
            g = g + ogain[...].astype(F32) * mm_nt(w1g, odn[...]) - c1g * s1
        piece(1, mm_tn(h1g if sec else h0g, g.astype(BF16)))
        gain_row = jnp.sum(mm_nt(own_w, dn_ref[...]) * state, axis=0, keepdims=True)
        sgn[0:1, :] = gain_row
        sgn[1:2, :] = jnp.full((1, feats), count, F32)

    @pl.when(first)
    def _():
        tail(0)

    @pl.when(s != 0)
    def _():
        tail(1)

    @pl.when(outer)
    def _():
        small_first().start()
        queue = [relay_copy(0), relay_copy(1), relay_copy(2)]
        queue += [up_copy(i) for i in range(quarter)]
        queue += [near_copy(k, j) for j in (1, 0) for k in range(1, hl)]
        for i in range(1, len(queue)):
            if i >= 2:
                queue[i - 2].wait_send()
            queue[i].start()
        for c in queue[max(0, len(queue) - 2):]:
            c.wait_send()

    @pl.when(jnp.logical_not(outer))
    def _():
        for i in range(quarter):
            up_copy(i).start()
        for k in range(1, hl):
            near_copy(k, 1).start()
        small_first().wait_recv()
        spr[...] = sgn[...] + rsm[...]
        for k in range(1, nd):
            small_copy(k).start()
        for g in range(3):
            relay_copy(g).wait_recv()
            for i in range(quarter):
                at = (near_far if g == 2 else deep_far) + i
                psum[g, i] = (sdp[at, 1 if g == 1 else 0].astype(F32) + relay[g, i].astype(F32)).astype(BF16)
                cross_copy(g, i).start()

    rgn_own = d // 2

    @pl.when(outer)
    def _():
        small_wait(rgn_own).wait_recv()
        spr[...] = rgn[rgn_own]

    small = spr[...]
    for j in range(1, nd // 2):
        p = lax.rem(rgn_own + j, nd // 2)
        small_wait(p).wait_recv()
        small = small + rgn[p]
    out[2 * part : 2 * part + 2, :] = small

    def total(j, from_pairs):
        sums = sdp[d, j].astype(F32)
        for k in range(1, hl):
            near_copy(k, j).wait_recv()
            sums = sums + rnear[j, k].astype(F32)
        if from_pairs:
            for m in range(nd // 4):
                cross_wait(j, m).wait_recv()
                sums = sums + rcross[j, m].astype(F32)
        else:
            for m in range(hl):
                up_wait(m).wait_recv()
                sums = sums + rfar[m].astype(F32)
        out[j * part : (j + 1) * part, :] = sums

    @pl.when(deep)
    def _():
        total(1, True)

    @pl.when(jnp.logical_not(deep))
    def _():
        total(1, False)

    total(0, True)

    @pl.when(outer)
    def _():
        small_first().wait_send()

    @pl.when(jnp.logical_not(outer))
    def _():
        for i in range(quarter):
            up_copy(i).wait_send()
            for g in range(3):
                cross_copy(g, i).wait_send()
        for k in range(1, hl):
            near_copy(k, 1).wait_send()
        for k in range(1, nd):
            small_copy(k).wait_send()
        for k in range(1, hl):
            near_copy(k, 0).wait_send()

    sib(0).wait_send()
    for k in range(1, nt):
        ab_scatter(k, s).wait_send()
        tok_own(k).wait_send()
        sq_own(k).wait_send()
    for k in range(nt):
        tok_cross(k).wait_send()
        for m in range(2):
            shared(m, k, s).wait_send()

    @pl.when(first)
    def _():
        ab_scatter(0, 0).wait_send()

    @pl.when(s != 0)
    def _():
        sib(1).wait_send()
        sib(2).wait_send()
        ab_gather(0, 0).wait_send()
        cd_gather(0, 0).wait_send()
        for k in range(1, nt):
            cd_scatter(k).wait_send()
            ab_gather(k, 1).wait_send()
            ab_forward(k).wait_send()
            cd_gather(k, 0).wait_send()
            cd_gather(k, 1).wait_send()
            for m in range(2):
                for b in range(2):
                    onward(m, k, b).wait_send()


def scale_kernel(part, sums, down_out, up_out, gain_out):
    scale = 1.0 / sums[2 * part + 1 : 2 * part + 2, :]
    down_out[...] = sums[0:part, :] * scale
    up_out[...] = sums[part : 2 * part, :] * scale
    gain_out[...] = sums[2 * part : 2 * part + 1, :] * scale


def solution(mesh):
    nt, nd, ns = mesh.shape["tensor"], mesh.shape["dp"], mesh.shape["section"]
    assert ns == 2 and nd % 4 == 0

    def local(inputs, down, up, gains, head, labels, valid):
        micro, per, feats = inputs.shape
        assert micro == ns
        tokens = micro * per
        rank = down.shape[2]
        own, rows, part = tokens // ns // nt, rank // nt, rank // nd
        wire = BF16 if own % 16 == 0 and rows % 16 == 0 else F32
        vmem = pl.BlockSpec(memory_space=pltpu.VMEM)
        dma = pltpu.SemaphoreType.DMA
        anyspace = pl.BlockSpec(memory_space=pl.ANY)
        sums = pl.pallas_call(
            functools.partial(kernel, nt, nd, feats * nt),
            out_shape=pltpu.VMEM((2 * part + 8, feats), F32),
            in_specs=[anyspace] * 7,
            out_specs=vmem,
            scratch_shapes=[
                pltpu.VMEM((tokens, feats), BF16),
                pltpu.VMEM((feats, rank), BF16),
                pltpu.VMEM((rank, feats), BF16),
                pltpu.VMEM((1, feats), BF16),
                pltpu.VMEM((feats, head.shape[1]), BF16),
                pltpu.VMEM((micro, per), jnp.int32),
                pltpu.VMEM((micro, per), jnp.int32),
                pltpu.VMEM((feats, rank), BF16),
                pltpu.VMEM((rank, feats), BF16),
                pltpu.VMEM((1, feats), BF16),
                pltpu.VMEM((2, nt, 3, own, rank), wire),
                pltpu.VMEM((2, nt, 3, own, rank), wire),
                pltpu.VMEM((16, tokens // 2), wire),
                pltpu.VMEM((nt, 16, tokens // 2), wire),
                pltpu.VMEM((nt, 4, rows, rank), wire),
                pltpu.VMEM((2, nt, 4, rows, rank), wire),
                pltpu.VMEM((6, rows, rank), wire),
                pltpu.VMEM((nt, 6, rows, rank), wire),
                pltpu.VMEM((6, own, rank), wire),
                pltpu.VMEM((2, nt, 6, own, rank), wire),
                pltpu.VMEM((nd, 2, part, feats), BF16),
                pltpu.VMEM((2, nd // 2, part, feats), BF16),
                pltpu.VMEM((nd // 2, part, feats), BF16),
                pltpu.VMEM((3, nd // 4, part, feats), BF16),
                pltpu.VMEM((3, nd // 4, part, feats), BF16),
                pltpu.VMEM((2, nd // 4, part, feats), BF16),
                pltpu.VMEM((2, feats), F32),
                pltpu.VMEM((2, feats), F32),
                pltpu.VMEM((2, feats), F32),
                pltpu.VMEM((nd // 2, 2, feats), F32),
                dma((7,)),
                dma((3,)), dma((3,)),
                dma((2, nt)), dma((2, nt)),
                dma((nt,)), dma((nt,)),
                dma((nt,)), dma((2, nt)),
                dma((nt,)), dma((nt,)),
                dma((nt,)), dma((nt,)),
                dma((nt,)), dma((nt,)),
                dma((2, nt)), dma((nt,)),
                dma((2, nt)), dma((2, 2, nt)),
                dma((2, 2, nt)), dma((2, 2, nt)),
                dma((2, nd // 2)), dma((2, nd // 2)),
                dma((nd // 4,)), dma((nd // 2,)),
                dma((3,)), dma((3,)),
                dma((3, nd // 4)), dma((2, nd // 4)),
                dma((nd,)), dma((nd // 2,)),
                dma, dma,
            ],
            compiler_params=pltpu.CompilerParams(collective_id=0, has_side_effects=True),
        )(inputs.reshape(tokens, feats), down[0], up[0], gains, head, labels, valid)
        down_t, up_g, gain_g = pl.pallas_call(
            functools.partial(scale_kernel, part),
            out_shape=(
                jax.ShapeDtypeStruct((part, feats), F32),
                jax.ShapeDtypeStruct((part, feats), F32),
                jax.ShapeDtypeStruct((1, feats), F32),
            ),
            in_specs=[vmem],
            out_specs=(vmem,) * 3,
        )(pltpu.with_memory_space_constraint(sums, pltpu.VMEM))
        return down_t.T[None], up_g[None], gain_g

    return jax.shard_map(
        local,
        mesh=mesh,
        in_specs=(
            P(None, "dp", "tensor"),
            P("section", "tensor", None),
            P("section", None, "tensor"),
            P("section", "tensor"),
            P("tensor", None),
            P(None, "dp"),
            P(None, "dp"),
        ),
        out_specs=(
            P("section", "tensor", "dp"),
            P("section", "dp", "tensor"),
            P("section", "tensor"),
        ),
        check_vma=False,
    )
```

```python
import functools

import jax
import jax.numpy as jnp
from jax import lax
from jax.experimental import pallas as pl
from jax.experimental.pallas import tpu as pltpu
from jax.sharding import PartitionSpec as P

MESH = pl.DeviceIdType.MESH
epsilon = 1e-05
F32 = jnp.float32
BF16 = jnp.bfloat16


def mm(a, b):
    return jnp.dot(a, b, preferred_element_type=F32)


def mm_nt(a, b):
    return lax.dot_general(a, b, (((1,), (1,)), ((), ())), preferred_element_type=F32)


def mm_tn(a, b):
    return lax.dot_general(a, b, (((0,), (0,)), ((), ())), preferred_element_type=F32)


def split(v):
    high = v.astype(BF16)
    return high, (v - high.astype(F32)).astype(BF16)


def kernel(
    nt, nd, width,
    x_hbm, dn_hbm, up_hbm, gain_hbm, head_hbm, lab_hbm, val_hbm,
    out,
    x_ref, dn_ref, up_ref, gain_ref, head_ref, lab_ref, val_ref,
    odn, oup, ogain, stok, rtok, ssq, rsq, sgram, rgram, pgram, gall, sres, res,
    sdp, rnear, rfar, relay, psum, rcross, sgn, rsm, spr, rgn,
    load, sib_s, sib_r, tok_s, tok_r, sq_s, sq_r, gr_s, gr_r, gq_s, gq_r, ga_s, ga_r, gf_s, gf_r, gc_s, gc_r,
    re_s, re_r, fw_s, fw_r, dp_s, dp_r, far_s, far_r, rel_s, rel_r, cr_s, cr_r, sm_s, sm_r, su_s, su_r,
):
    s, d, t = lax.axis_index("section"), lax.axis_index("dp"), lax.axis_index("tensor")
    first = s == 0
    tokens, feats = x_ref.shape
    rank = dn_ref.shape[1]
    half = tokens // 2
    own = half // nt
    rows = rank // nt
    part = rank // nd
    wire = stok.dtype

    hl = nd // 2
    quarter = hl // 2
    side = d // hl
    local_d = lax.rem(d, hl)
    far = (1 - side) * hl
    odd = lax.rem(d, 2)
    outer = odd == side
    deep = local_d // quarter == side
    tip = jnp.logical_and(outer, deep)
    partner = d + 1 - 2 * odd

    def ahead(k):
        return lax.rem(t + k, nt)

    def behind(k):
        return lax.rem(t + nt - k, nt)

    loads = [
        pltpu.make_async_copy(a, b, load.at[i])
        for i, (a, b) in enumerate((
            (up_hbm, up_ref), (head_hbm, head_ref), (x_hbm, x_ref), (gain_hbm, gain_ref),
            (dn_hbm, dn_ref), (lab_hbm, lab_ref), (val_hbm, val_ref),
        ))
    ]
    for c in loads:
        c.start()

    barrier = pltpu.get_barrier_semaphore()
    for k in range(1, nd):
        to = lax.rem(d + k, nd)

        @pl.when(jnp.logical_not(jnp.logical_and(tip, to == nd - 1 - d)))
        def _():
            pl.semaphore_signal(barrier, inc=1, device_id=(s, to, t), device_id_type=MESH)

    group = [(k, o) for k in range(nt) for o in (0, 1) if (k, o) != (0, 0)]
    for k, o in group:
        pl.semaphore_signal(barrier, inc=1, device_id=(1 - s if o else s, d, ahead(k)), device_id_type=MESH)

    def copy(src, dst, ss, rs, section, column):
        return pltpu.make_async_remote_copy(
            src_ref=src, dst_ref=dst, send_sem=ss, recv_sem=rs, device_id=(section, d, column), device_id_type=MESH
        )

    def whole(ref, sem):
        return copy(ref, ref, sem, sem, 1 - s, t)

    def arrived(ref, sem):
        whole(ref, sem).wait_recv()

    def sent(ref, sem):
        whole(ref, sem).wait_send()

    def put_gram(j, g):
        g = g.astype(wire)
        for i in range(nt):
            sgram[i, j] = g[i * rows : (i + 1) * rows]

    loads[0].wait()
    up = up_ref[...]
    put_gram(0, mm_nt(up, up))
    loads[1].wait()
    head = head_ref[...]
    put_gram(1, mm(up, head))

    pl.semaphore_wait(barrier, len(group) + nd - 1 - tip.astype(jnp.int32))

    def sib(i):
        a, b = ((up_ref, oup), (dn_ref, odn), (gain_ref, ogain))[i]
        return copy(a, b, sib_s.at[i], sib_r.at[i], 1 - s, t)

    def ab_scatter(k, sender):
        return copy(
            sgram.at[ahead(k), pl.ds(0, 2)], rgram.at[sender, k, pl.ds(0, 2)], gr_s, gr_r.at[sender], 1, ahead(k)
        )

    def cd_scatter(k):
        return copy(sgram.at[ahead(k), pl.ds(2, 2)], rgram.at[1, k, pl.ds(2, 2)], gq_s, gq_r, 1, ahead(k))

    def tok_cross(k):
        block = pl.ds(0, 2)
        return copy(
            stok.at[1 - s, ahead(k), block], rtok.at[1, k, block], tok_s.at[1], tok_r.at[1], 1 - s, ahead(k)
        )

    def tok_own(k):
        return copy(stok.at[s, ahead(k)], rtok.at[0, k], tok_s.at[0], tok_r.at[0], s, ahead(k))

    def sq_own(k):
        return copy(ssq, rsq.at[k], sq_s, sq_r, s, ahead(k))

    ab_all = gall.at[:, pl.ds(0, 4)]
    cd_all = gall.at[:, pl.ds(4, 2)]

    def ab_gather(k):
        block = pl.ds(0, 4)
        return copy(pgram.at[block], gall.at[t, block], ga_s, ga_r, 1, ahead(k))

    def ab_forward():
        return copy(ab_all, ab_all, gf_s, gf_r, 0, t)

    def cd_gather(k, section):
        block = pl.ds(4, 2)
        return copy(pgram.at[block], gall.at[t, block], gc_s.at[section], gc_r, section, ahead(k))

    sib(0).start()
    for k in range(1, nt):
        ab_scatter(k, s).start()

    @pl.when(first)
    def _():
        ab_scatter(0, 0).start()

    for c in loads[2:]:
        c.wait()
    gain = gain_ref[...].astype(F32)
    xb = x_ref[...]
    xf = xb.astype(F32)
    xup = mm_nt(xb, up).astype(wire)
    proj = mm((xf * gain).astype(BF16), dn_ref[...]).astype(wire)
    for b in range(2):
        for i in range(nt):
            at = b * half + i * own
            stok[b, i, 0] = proj[at : at + own]
            stok[b, i, 1] = xup[at : at + own]
    for k in range(nt):
        tok_cross(k).start()

    xm = x_ref[pl.ds(pl.multiple_of(s * half, half), half), :]
    xmf = xm.astype(F32)
    xhead = mm(xm, head).astype(wire)
    for i in range(nt):
        stok[s, i, 2] = xhead[i * own : (i + 1) * own]
    ones = jnp.ones((8, feats), BF16)
    square_h, square_l = split(xmf * xmf)
    row_h, row_l = split(mm_nt(ones, square_h) + mm_nt(ones, square_l))
    ssq[0:8] = row_h.astype(wire)
    ssq[8:16] = row_l.astype(wire)

    @pl.when(s != 0)
    def _():
        sib(0).wait_recv()
        other = oup[...]
        put_gram(2, mm_nt(other, up))
        put_gram(3, mm((other.astype(F32) * gain).astype(BF16), dn_ref[...]))
        for k in range(1, nt):
            cd_scatter(k).start()

    for k in range(1, nt):
        tok_own(k).start()
        sq_own(k).start()

    @pl.when(s != 0)
    def _():
        sib(1).start()
        sib(2).start()
        arrived(rgram.at[1, pl.ds(1, nt - 1), pl.ds(0, 2)], gr_r.at[1])
        mine1 = sgram[t, 0:2].astype(F32)
        for k in range(1, nt):
            mine1 = mine1 + rgram[1, k, 0:2].astype(F32)
        arrived(rgram.at[0, :, pl.ds(0, 2)], gr_r.at[0])
        mine0 = rgram[0, 0, 0:2].astype(F32)
        for k in range(1, nt):
            mine0 = mine0 + rgram[0, k, 0:2].astype(F32)
        for j, v in ((0, mine0.astype(wire)), (2, mine1.astype(wire))):
            pgram[j : j + 2] = v
            gall[t, j : j + 2] = v
        for k in range(1, nt):
            ab_gather(k).start()
        arrived(rgram.at[1, pl.ds(1, nt - 1), pl.ds(2, 2)], gq_r)
        both = sgram[t, 2:4].astype(F32)
        for k in range(1, nt):
            both = both + rgram[1, k, 2:4].astype(F32)
        both = both.astype(wire)
        pgram[4:6] = both
        gall[t, 4:6] = both
        for k in range(1, nt):
            cd_gather(k, 1).start()
        for k in range(nt):
            cd_gather(k, 0).start()

    lab = jnp.where(first, lab_ref[0:1, :], lab_ref[1:2, :])
    val = jnp.where(first, val_ref[0:1, :], val_ref[1:2, :]).astype(F32)
    labels_n = head.shape[1]
    hot_t = jnp.where(lax.broadcasted_iota(jnp.int32, (labels_n, half), 0) == lab, val, 0.0).astype(BF16)
    val_t = jnp.broadcast_to(val, (labels_n, half)).astype(BF16)
    chosen = (
        lax.broadcasted_iota(jnp.int32, (own, half), 0) + t * own
        == lax.broadcasted_iota(jnp.int32, (own, half), 1)
    )
    pick = chosen.astype(F32).astype(BF16)
    onehot = mm_nt(pick, hot_t)
    validity = mm_nt(pick, val_t)
    count = jnp.sum(val_ref[...].astype(F32))

    arrived(rtok.at[0, pl.ds(1, nt - 1)], tok_r.at[0])
    mine = stok[s, t].astype(F32)
    for k in range(1, nt):
        mine = mine + rtok[0, k].astype(F32)
    arrived(rtok.at[1, :, pl.ds(0, 2)], tok_r.at[1])
    theirs = rtok[1, 0, 0:2].astype(F32)
    for k in range(1, nt):
        theirs = theirs + rtok[1, k, 0:2].astype(F32)
    p0 = jnp.where(first, mine[0], theirs[0])
    p1 = jnp.where(first, theirs[0], mine[0])
    v0 = jnp.where(first, mine[1], theirs[1])
    v1 = jnp.where(first, theirs[1], mine[1])
    xh = mine[2]
    arrived(rsq.at[pl.ds(1, nt - 1)], sq_r)
    sq = ssq[...].astype(F32)
    for k in range(1, nt):
        sq = sq + rsq[k].astype(F32)

    def rowsum(v):
        return jnp.sum(v, axis=1, keepdims=True)

    sq0 = rowsum(jnp.where(chosen, sq[0:1] + sq[8:9], 0.0))
    inv0 = lax.rsqrt(sq0 / width + epsilon)
    pre0 = inv0 * p0
    sig0 = jax.nn.sigmoid(pre0)
    h0 = (pre0 * sig0).astype(BF16)
    h0f = h0.astype(F32)

    @pl.when(s != 0)
    def _():
        arrived(gall.at[pl.ds(1, nt - 1), pl.ds(0, 4)], ga_r)
        ab_forward().start()
        arrived(gall.at[pl.ds(1, nt - 1), pl.ds(4, 2)], gc_r)

    @pl.when(first)
    def _():
        ab_forward().wait_recv()
        arrived(cd_all, gc_r)

    def gram(j):
        return gall[:, j].reshape(rank, rank).astype(BF16)

    a0, b0, a1, b1, c0, d1 = (gram(j) for j in range(6))

    parts = ((0, 2), (2, 4))

    def keep(j, v):
        v = v.astype(wire)
        sres[j] = v
        res[s, t, j] = v

    def shared(m, k):
        at, size = parts[m]
        span = pl.ds(at, size)
        return copy(sres.at[span], res.at[s, t, span], re_s.at[m], re_r.at[m, s], 1, ahead(k))

    def onward(m, b):
        at, size = parts[m]
        block = res.at[b, :, pl.ds(at, size)]
        return copy(block, block, fw_s.at[m], fw_r.at[m], 0, t)

    def share(m):
        for k in range(1, nt):
            shared(m, k).start()

        @pl.when(first)
        def _():
            shared(m, 0).start()

    h0a = mm(h0, a0)
    p1 = p1 + mm(h0, d1)
    s1u0 = v0 + h0a
    s1u1 = v1 + mm(h0, c0)
    base = xh + mm(h0, b0)
    sq1 = sq0 + rowsum(h0f * (v0 + s1u0))
    inv1 = lax.rsqrt(sq1 / width + epsilon)
    pre1 = inv1 * p1
    sig1 = jax.nn.sigmoid(pre1)
    h1 = (pre1 * sig1).astype(BF16)
    h1f = h1.astype(F32)
    keep(0, h0)
    keep(1, h1)
    share(0)
    yu1 = s1u1 + mm(h1, a1)
    yu0 = s1u0 + mm_nt(h1, c0)
    base = base + mm(h1, b1)
    sq2 = sq1 + rowsum(h1f * (s1u1 + yu1))
    inv2 = lax.rsqrt(sq2 / width + epsilon)
    logits = inv2 * base
    expo = jnp.exp(logits - jnp.max(logits, axis=1, keepdims=True))
    cot = expo / rowsum(expo) * validity - onehot
    radial = rowsum(cot * base)
    wh = (inv2 * cot).astype(BF16)
    keep(2, wh)
    ch = inv2 * inv2 * inv2 / width * radial
    hg1 = mm_nt(wh, b1) - ch * yu1
    act1 = hg1 * sig1 * (1.0 + pre1 * (1.0 - sig1))
    w1 = (inv1 * act1).astype(BF16)
    c1 = inv1 * inv1 * inv1 / width * rowsum(act1 * p1)
    ch_h, ch_l = split(ch)
    c1_h, c1_l = split(c1)
    lane = lax.broadcasted_iota(jnp.int32, (own, rank), 1)
    q4 = rank // 4
    keep(3, w1)
    keep(4, jnp.where(
        lane < q4, ch_h.astype(F32),
        jnp.where(lane < 2 * q4, ch_l.astype(F32), jnp.where(lane < 3 * q4, c1_h.astype(F32), c1_l.astype(F32))),
    ))
    hg0 = mm_nt(wh, b0) - ch * yu0 + mm_nt(w1, d1) - c1 * s1u0
    act0 = hg0 * sig0 * (1.0 + pre0 * (1.0 - sig0))
    w0 = (inv0 * act0).astype(BF16)
    keep(5, w0)
    share(1)

    def got(j):
        return res[:, :, j].reshape(tokens, res.shape[-1])

    def piece(j, full):
        full = full.astype(BF16)
        for i in range(nd):
            sdp[i, j] = full[i * part : (i + 1) * part]

    near_far = far + side * quarter
    deep_far = far + (1 - side) * quarter

    def remote(src, dst, ss, rs, to):
        return pltpu.make_async_remote_copy(
            src_ref=src, dst_ref=dst, send_sem=ss, recv_sem=rs, device_id=(s, to, t), device_id_type=MESH
        )

    def near_copy(k, j):
        to = side * hl + lax.rem(local_d + k, hl)
        return remote(sdp.at[to, j], rnear.at[j, k], dp_s.at[j, k - 1], dp_r.at[j], to)

    def up_copy(i):
        return remote(sdp.at[near_far + i, 1], rfar.at[local_d], far_s.at[i], far_r, near_far + i)

    def relay_copy(g):
        block = pl.ds(near_far if g == 2 else deep_far, quarter)
        return remote(sdp.at[block, 1 if g == 1 else 0], relay.at[g], rel_s.at[g], rel_r.at[g], partner)

    def cross_copy(g, i):
        m = local_d // 2
        to = (near_far if g == 2 else deep_far) + i
        return remote(psum.at[g, i], rcross.at[1 if g == 1 else 0, m], cr_s, cr_r.at[1 if g == 1 else 0], to)

    def small_copy(k):
        to = lax.rem(d + k, nd)
        return remote(spr, rgn.at[d // 2], sm_s, sm_r.at[(to // 2 != d // 2).astype(jnp.int32)], to)

    def small_first():
        return remote(sgn, rsm, su_s, su_r, partner)

    def tail(sec):
        u0, u1 = (oup, up_ref) if sec else (up_ref, oup)

        def collect(m):
            at, size = parts[m]
            span = pl.ds(at, size)
            if sec:
                arrived(res.at[1, pl.ds(1, nt - 1), span], re_r.at[m, 1])
                onward(m, 1).start()
                arrived(res.at[0, :, span], re_r.at[m, 0])
                onward(m, 0).start()
            else:
                arrived(res.at[:, :, span], fw_r.at[m])

        if sec == 0:
            for i in range(3):
                sib(i).wait_recv()
        collect(0)
        h0g, h1g = got(0).astype(BF16), got(1).astype(BF16)
        s1 = xf + mm(h0g, u0[...])
        y = s1 + mm(h1g, u1[...])
        collect(1)
        w1g = got(3).astype(BF16)
        state, own_w = (s1, w1g) if sec else (xf, got(5).astype(BF16))
        piece(0, mm_tn(own_w, (state * gain).astype(BF16)))

        @pl.when(outer)
        def _():
            relay_copy(0).start()

        @pl.when(jnp.logical_not(outer))
        def _():
            for k in range(1, hl):
                near_copy(k, 0).start()

        cg = got(4).astype(F32)
        chg = cg[:, 0:1] + cg[:, q4 : q4 + 1]
        g = mm_nt(got(2).astype(BF16), head_ref[...]) - chg * y
        if sec == 0:
            c1g = cg[:, 2 * q4 : 2 * q4 + 1] + cg[:, 3 * q4 : 3 * q4 + 1]
            g = g + ogain[...].astype(F32) * mm_nt(w1g, odn[...]) - c1g * s1
        piece(1, mm_tn(h1g if sec else h0g, g.astype(BF16)))
        gain_row = jnp.sum(mm_nt(own_w, dn_ref[...]) * state, axis=0, keepdims=True)
        sgn[0:1, :] = gain_row
        sgn[1:2, :] = jnp.full((1, feats), count, F32)

    @pl.when(first)
    def _():
        tail(0)

    @pl.when(s != 0)
    def _():
        tail(1)

    @pl.when(outer)
    def _():
        small_first().start()
        queue = [relay_copy(0), relay_copy(1), relay_copy(2)]
        queue += [up_copy(i) for i in range(quarter)]
        queue += [near_copy(k, j) for j in (1, 0) for k in range(1, hl)]
        for i in range(1, len(queue)):
            if i >= 2:
                queue[i - 2].wait_send()
            queue[i].start()
        for c in queue[max(0, len(queue) - 2):]:
            c.wait_send()

    @pl.when(jnp.logical_not(outer))
    def _():
        for i in range(quarter):
            up_copy(i).start()
        for k in range(1, hl):
            near_copy(k, 1).start()
        small_first().wait_recv()
        spr[...] = sgn[...] + rsm[...]
        for k in range(1, nd):
            small_copy(k).start()
        for g in range(3):
            relay_copy(g).wait_recv()
            for i in range(quarter):
                at = (near_far if g == 2 else deep_far) + i
                psum[g, i] = (sdp[at, 1 if g == 1 else 0].astype(F32) + relay[g, i].astype(F32)).astype(BF16)
                cross_copy(g, i).start()

    rgn_own = d // 2

    @pl.when(outer)
    def _():
        arrived(rgn.at[rgn_own], sm_r.at[0])
        spr[...] = rgn[rgn_own]

    arrived(rgn.at[pl.ds(1, nd // 2 - 1)], sm_r.at[1])
    small = spr[...]
    for j in range(1, nd // 2):
        p = lax.rem(rgn_own + j, nd // 2)
        small = small + rgn[p]
    out[2 * part : 2 * part + 2, :] = small

    def total(j, from_pairs):
        arrived(rnear.at[j, pl.ds(1, hl - 1)], dp_r.at[j])
        sums = sdp[d, j].astype(F32)
        for k in range(1, hl):
            sums = sums + rnear[j, k].astype(F32)
        if from_pairs:
            arrived(rcross.at[j], cr_r.at[j])
            for m in range(nd // 4):
                sums = sums + rcross[j, m].astype(F32)
        else:
            arrived(rfar, far_r)
            for m in range(hl):
                sums = sums + rfar[m].astype(F32)
        out[j * part : (j + 1) * part, :] = sums

    @pl.when(deep)
    def _():
        total(1, True)

    @pl.when(jnp.logical_not(deep))
    def _():
        total(1, False)

    total(0, True)

    @pl.when(outer)
    def _():
        small_first().wait_send()

    @pl.when(jnp.logical_not(outer))
    def _():
        for i in range(quarter):
            up_copy(i).wait_send()
        sent(psum, cr_s)
        for k in range(1, hl):
            near_copy(k, 1).wait_send()
            near_copy(k, 0).wait_send()
        sent(rgn.at[pl.ds(1, nd - 1)], sm_s)

    sib(0).wait_send()
    sent(rtok.at[0, pl.ds(1, nt - 1)], tok_s.at[0])
    sent(rtok.at[1, :, pl.ds(0, 2)], tok_s.at[1])
    sent(rsq.at[pl.ds(1, nt - 1)], sq_s)

    @pl.when(first)
    def _():
        sent(rgram.at[0, :, pl.ds(0, 2)], gr_s)
        for m, (at, size) in enumerate(parts):
            sent(res.at[0, :, pl.ds(at, size)], re_s.at[m])

    @pl.when(s != 0)
    def _():
        sib(1).wait_send()
        sib(2).wait_send()
        sent(rgram.at[1, pl.ds(1, nt - 1), pl.ds(0, 2)], gr_s)
        sent(rgram.at[1, pl.ds(1, nt - 1), pl.ds(2, 2)], gq_s)
        sent(gall.at[pl.ds(1, nt - 1), pl.ds(0, 4)], ga_s)
        ab_forward().wait_send()
        sent(cd_all, gc_s.at[0])
        sent(gall.at[pl.ds(1, nt - 1), pl.ds(4, 2)], gc_s.at[1])
        for m, (at, size) in enumerate(parts):
            sent(res.at[1, pl.ds(1, nt - 1), pl.ds(at, size)], re_s.at[m])
            sent(res.at[:, :, pl.ds(at, size)], fw_s.at[m])


def scale_kernel(part, sums, down_out, up_out, gain_out):
    scale = 1.0 / sums[2 * part + 1 : 2 * part + 2, :]
    down_out[...] = sums[0:part, :] * scale
    up_out[...] = sums[part : 2 * part, :] * scale
    gain_out[...] = sums[2 * part : 2 * part + 1, :] * scale


def solution(mesh):
    nt, nd, ns = mesh.shape["tensor"], mesh.shape["dp"], mesh.shape["section"]
    assert ns == 2 and nd % 4 == 0

    def local(inputs, down, up, gains, head, labels, valid):
        micro, per, feats = inputs.shape
        assert micro == ns
        tokens = micro * per
        rank = down.shape[2]
        own, rows, part = tokens // ns // nt, rank // nt, rank // nd
        wire = BF16 if own % 16 == 0 and rows % 16 == 0 else F32
        vmem = pl.BlockSpec(memory_space=pltpu.VMEM)
        dma = pltpu.SemaphoreType.DMA
        anyspace = pl.BlockSpec(memory_space=pl.ANY)
        sums = pl.pallas_call(
            functools.partial(kernel, nt, nd, feats * nt),
            out_shape=pltpu.VMEM((2 * part + 8, feats), F32),
            in_specs=[anyspace] * 7,
            out_specs=vmem,
            scratch_shapes=[
                pltpu.VMEM((tokens, feats), BF16),
                pltpu.VMEM((feats, rank), BF16),
                pltpu.VMEM((rank, feats), BF16),
                pltpu.VMEM((1, feats), BF16),
                pltpu.VMEM((feats, head.shape[1]), BF16),
                pltpu.VMEM((micro, per), jnp.int32),
                pltpu.VMEM((micro, per), jnp.int32),
                pltpu.VMEM((feats, rank), BF16),
                pltpu.VMEM((rank, feats), BF16),
                pltpu.VMEM((1, feats), BF16),
                pltpu.VMEM((2, nt, 3, own, rank), wire),
                pltpu.VMEM((2, nt, 3, own, rank), wire),
                pltpu.VMEM((16, tokens // 2), wire),
                pltpu.VMEM((nt, 16, tokens // 2), wire),
                pltpu.VMEM((nt, 4, rows, rank), wire),
                pltpu.VMEM((2, nt, 4, rows, rank), wire),
                pltpu.VMEM((6, rows, rank), wire),
                pltpu.VMEM((nt, 6, rows, rank), wire),
                pltpu.VMEM((6, own, rank), wire),
                pltpu.VMEM((2, nt, 6, own, rank), wire),
                pltpu.VMEM((nd, 2, part, feats), BF16),
                pltpu.VMEM((2, nd // 2, part, feats), BF16),
                pltpu.VMEM((nd // 2, part, feats), BF16),
                pltpu.VMEM((3, nd // 4, part, feats), BF16),
                pltpu.VMEM((3, nd // 4, part, feats), BF16),
                pltpu.VMEM((2, nd // 4, part, feats), BF16),
                pltpu.VMEM((2, feats), F32),
                pltpu.VMEM((2, feats), F32),
                pltpu.VMEM((2, feats), F32),
                pltpu.VMEM((nd, 2, feats), F32),
                dma((7,)),
                dma((3,)), dma((3,)),
                dma((2,)), dma((2,)),
                dma, dma,
                dma, dma((2,)),
                dma, dma,
                dma, dma,
                dma, dma,
                dma((2,)), dma,
                dma((2,)), dma((2, 2)),
                dma((2,)), dma((2,)),
                dma((2, nd // 2 - 1)), dma((2,)),
                dma((nd // 4,)), dma,
                dma((3,)), dma((3,)),
                dma, dma((2,)),
                dma, dma((2,)),
                dma, dma,
            ],
            compiler_params=pltpu.CompilerParams(collective_id=0, has_side_effects=True),
        )(inputs.reshape(tokens, feats), down[0], up[0], gains, head, labels, valid)
        down_t, up_g, gain_g = pl.pallas_call(
            functools.partial(scale_kernel, part),
            out_shape=(
                jax.ShapeDtypeStruct((part, feats), F32),
                jax.ShapeDtypeStruct((part, feats), F32),
                jax.ShapeDtypeStruct((1, feats), F32),
            ),
            in_specs=[vmem],
            out_specs=(vmem,) * 3,
        )(pltpu.with_memory_space_constraint(sums, pltpu.VMEM))
        return down_t.T[None], up_g[None], gain_g

    return jax.shard_map(
        local,
        mesh=mesh,
        in_specs=(
            P(None, "dp", "tensor"),
            P("section", "tensor", None),
            P("section", None, "tensor"),
            P("section", "tensor"),
            P("tensor", None),
            P(None, "dp"),
            P(None, "dp"),
        ),
        out_specs=(
            P("section", "tensor", "dp"),
            P("section", "dp", "tensor"),
            P("section", "tensor"),
        ),
        check_vma=False,
    )
```

```python
import functools

import jax
import jax.numpy as jnp
from jax import lax
from jax.experimental import pallas as pl
from jax.experimental.pallas import tpu as pltpu
from jax.sharding import PartitionSpec as P

MESH = pl.DeviceIdType.MESH
epsilon = 1e-05
F32 = jnp.float32
BF16 = jnp.bfloat16


def mm(a, b):
    return jnp.dot(a, b, preferred_element_type=F32)


def mm_nt(a, b):
    return lax.dot_general(a, b, (((1,), (1,)), ((), ())), preferred_element_type=F32)


def mm_tn(a, b):
    return lax.dot_general(a, b, (((0,), (0,)), ((), ())), preferred_element_type=F32)


def split(v):
    high = v.astype(BF16)
    return high, (v - high.astype(F32)).astype(BF16)


def kernel(
    nt, nd, width,
    x_hbm, dn_hbm, up_hbm, gain_hbm, head_hbm, lab_hbm, val_hbm,
    out,
    x_ref, dn_ref, up_ref, gain_ref, head_ref, lab_ref, val_ref,
    odn, oup, ogain, stok, rtok, ssq, rsq, sgram, rgram, pgram, gall, sres, res,
    sdp, rnear, rfar, relay, psum, rcross, sgn, rsm, spr, rgn,
    bulk, load, plane_s, sib_s, sib_r, tok_r, gr_r, gq_r, ga_r, gf_r, gc_r, re_r, fw_r, la_r, dp_s, dp_r, far_s, far_r, rel_s, rel_r, cr_s, cr_r, sm_s, sm_r, su_s, su_r,
):
    s, d, t = lax.axis_index("section"), lax.axis_index("dp"), lax.axis_index("tensor")
    first = s == 0
    tokens, feats = x_ref.shape
    rank = dn_ref.shape[1]
    half = tokens // 2
    own = half // nt
    rows = rank // nt
    part = rank // nd
    wire = stok.dtype
    own_size, rows_size = (n * rank * wire.itemsize for n in (own, rows))
    tok_size = (3 * (nt - 1) + 2 * nt) * own_size + (nt - 1) * 16 * half * wire.itemsize

    hl = nd // 2
    quarter = hl // 2
    side = d // hl
    local_d = lax.rem(d, hl)
    far = (1 - side) * hl
    odd = lax.rem(d, 2)
    outer = odd == side
    deep = local_d // quarter == side
    tip = jnp.logical_and(outer, deep)
    partner = d + 1 - 2 * odd

    def ahead(k):
        return lax.rem(t + k, nt)

    def behind(k):
        return lax.rem(t + nt - k, nt)

    loads = [
        pltpu.make_async_copy(a, b, load.at[min(i, 5)])
        for i, (a, b) in enumerate((
            (up_hbm, up_ref), (head_hbm, head_ref), (gain_hbm, gain_ref), (lab_hbm, lab_ref), (val_hbm, val_ref),
            (x_hbm, x_ref), (dn_hbm, dn_ref),
        ))
    ]
    for c in loads:
        c.start()

    barrier = pltpu.get_barrier_semaphore()
    for k in range(1, nd):
        to = lax.rem(d + k, nd)

        @pl.when(jnp.logical_not(jnp.logical_and(tip, to == nd - 1 - d)))
        def _():
            pl.semaphore_signal(barrier, inc=1, device_id=(s, to, t), device_id_type=MESH)

    group = [(k, o) for k in range(nt) for o in (0, 1) if (k, o) != (0, 0)]
    for k, o in group:
        pl.semaphore_signal(barrier, inc=1, device_id=(1 - s if o else s, d, ahead(k)), device_id_type=MESH)

    def copy(src, dst, ss, rs, section, column):
        return pltpu.make_async_remote_copy(
            src_ref=src, dst_ref=dst, send_sem=ss, recv_sem=rs, device_id=(section, d, column), device_id_type=MESH
        )

    def block(size):
        return bulk.at[pl.ds(0, size // (4 * bulk.shape[1] * bulk.shape[2]))]

    def whole(ref, sem):
        return copy(ref, ref, sem, sem, 1 - s, t)

    def arrived(ref, sem):
        whole(ref, sem).wait_recv()

    def sent(ref, sem):
        whole(ref, sem).wait_send()

    def put_gram(j, g):
        g = g.astype(wire)
        for i in range(nt):
            sgram[i, j] = g[i * rows : (i + 1) * rows]

    loads[0].wait()
    up = up_ref[...]
    put_gram(0, mm_nt(up, up))
    loads[1].wait()
    head = head_ref[...]
    put_gram(1, mm(up, head))

    pl.semaphore_wait(barrier, len(group) + nd - 1 - tip.astype(jnp.int32))

    def sib(i):
        a, b = ((up_ref, oup), (dn_ref, odn), (gain_ref, ogain))[i]
        return copy(a, b, sib_s if i == 2 else plane_s, sib_r.at[i], 1 - s, t)

    def ab_scatter(k, sender):
        return copy(
            sgram.at[ahead(k), pl.ds(0, 2)], rgram.at[sender, k, pl.ds(0, 2)], plane_s, gr_r, 1, ahead(k)
        )

    def cd_scatter(k):
        return copy(sgram.at[ahead(k), pl.ds(2, 2)], rgram.at[1, k, pl.ds(2, 2)], plane_s, gq_r, 1, ahead(k))

    def tok_cross(k):
        block = pl.ds(0, 2)
        return copy(
            stok.at[1 - s, ahead(k), block], rtok.at[1, k, block], plane_s, tok_r, 1 - s, ahead(k)
        )

    def tok_own(k):
        return copy(stok.at[s, ahead(k)], rtok.at[0, k], plane_s, tok_r, s, ahead(k))

    def sq_own(k):
        return copy(ssq, rsq.at[k], plane_s, tok_r, s, ahead(k))

    ab_all = gall.at[:, pl.ds(0, 4)]
    cd_all = gall.at[:, pl.ds(4, 2)]

    def ab_gather(k):
        block = pl.ds(0, 4)
        return copy(pgram.at[block], gall.at[t, block], plane_s, ga_r, 1, ahead(k))

    def ab_forward():
        return copy(ab_all, ab_all, plane_s, gf_r, 0, t)

    def cd_gather(k, section):
        block = pl.ds(4, 2)
        return copy(pgram.at[block], gall.at[t, block], plane_s, gc_r, section, ahead(k))

    sib(0).start()
    for k in range(1, nt):
        ab_scatter(k, s).start()

    @pl.when(first)
    def _():
        ab_scatter(0, 0).start()

    for c in loads[2:5]:
        c.wait()
    pltpu.make_async_copy(block(2 * tokens * feats + 2 * rank * feats), block(2 * tokens * feats + 2 * rank * feats), load.at[5]).wait()
    gain = gain_ref[...].astype(F32)
    xb = x_ref[...]
    xf = xb.astype(F32)
    xup = mm_nt(xb, up).astype(wire)
    proj = mm((xf * gain).astype(BF16), dn_ref[...]).astype(wire)
    for b in range(2):
        for i in range(nt):
            at = b * half + i * own
            stok[b, i, 0] = proj[at : at + own]
            stok[b, i, 1] = xup[at : at + own]
    for k in range(nt):
        tok_cross(k).start()

    xm = x_ref[pl.ds(pl.multiple_of(s * half, half), half), :]
    xmf = xm.astype(F32)
    xhead = mm(xm, head).astype(wire)
    for i in range(nt):
        stok[s, i, 2] = xhead[i * own : (i + 1) * own]
    ones = jnp.ones((8, feats), BF16)
    square_h, square_l = split(xmf * xmf)
    row_h, row_l = split(mm_nt(ones, square_h) + mm_nt(ones, square_l))
    ssq[0:8] = row_h.astype(wire)
    ssq[8:16] = row_l.astype(wire)

    @pl.when(s != 0)
    def _():
        sib(0).wait_recv()
        other = oup[...]
        put_gram(2, mm_nt(other, up))
        put_gram(3, mm((other.astype(F32) * gain).astype(BF16), dn_ref[...]))
        for k in range(1, nt):
            cd_scatter(k).start()

    for k in range(1, nt):
        tok_own(k).start()
        sq_own(k).start()

    @pl.when(s != 0)
    def _():
        sib(1).start()
        sib(2).start()
        arrived(block((2 * nt - 1) * 2 * rows_size), gr_r)
        mine1 = sgram[t, 0:2].astype(F32)
        for k in range(1, nt):
            mine1 = mine1 + rgram[1, k, 0:2].astype(F32)
        mine0 = rgram[0, 0, 0:2].astype(F32)
        for k in range(1, nt):
            mine0 = mine0 + rgram[0, k, 0:2].astype(F32)
        for j, v in ((0, mine0.astype(wire)), (2, mine1.astype(wire))):
            pgram[j : j + 2] = v
            gall[t, j : j + 2] = v
        for k in range(1, nt):
            ab_gather(k).start()
        arrived(rgram.at[1, pl.ds(1, nt - 1), pl.ds(2, 2)], gq_r)
        both = sgram[t, 2:4].astype(F32)
        for k in range(1, nt):
            both = both + rgram[1, k, 2:4].astype(F32)
        both = both.astype(wire)
        pgram[4:6] = both
        gall[t, 4:6] = both
        for k in range(1, nt):
            cd_gather(k, 1).start()
        for k in range(nt):
            cd_gather(k, 0).start()

    lab = jnp.where(first, lab_ref[0:1, :], lab_ref[1:2, :])
    val = jnp.where(first, val_ref[0:1, :], val_ref[1:2, :]).astype(F32)
    labels_n = head.shape[1]
    hot_t = jnp.where(lax.broadcasted_iota(jnp.int32, (labels_n, half), 0) == lab, val, 0.0).astype(BF16)
    val_t = jnp.broadcast_to(val, (labels_n, half)).astype(BF16)
    chosen = (
        lax.broadcasted_iota(jnp.int32, (own, half), 0) + t * own
        == lax.broadcasted_iota(jnp.int32, (own, half), 1)
    )
    pick = chosen.astype(F32).astype(BF16)
    onehot = mm_nt(pick, hot_t)
    validity = mm_nt(pick, val_t)
    count = jnp.sum(val_ref[...].astype(F32))

    arrived(block(tok_size), tok_r)
    mine = stok[s, t].astype(F32)
    for k in range(1, nt):
        mine = mine + rtok[0, k].astype(F32)
    theirs = rtok[1, 0, 0:2].astype(F32)
    for k in range(1, nt):
        theirs = theirs + rtok[1, k, 0:2].astype(F32)
    p0 = jnp.where(first, mine[0], theirs[0])
    p1 = jnp.where(first, theirs[0], mine[0])
    v0 = jnp.where(first, mine[1], theirs[1])
    v1 = jnp.where(first, theirs[1], mine[1])
    xh = mine[2]
    sq = ssq[...].astype(F32)
    for k in range(1, nt):
        sq = sq + rsq[k].astype(F32)

    def rowsum(v):
        return jnp.sum(v, axis=1, keepdims=True)

    sq0 = rowsum(jnp.where(chosen, sq[0:1] + sq[8:9], 0.0))
    inv0 = lax.rsqrt(sq0 / width + epsilon)
    pre0 = inv0 * p0
    sig0 = jax.nn.sigmoid(pre0)
    h0 = (pre0 * sig0).astype(BF16)
    h0f = h0.astype(F32)

    @pl.when(s != 0)
    def _():
        arrived(gall.at[pl.ds(1, nt - 1), pl.ds(0, 4)], ga_r)
        ab_forward().start()
        arrived(gall.at[pl.ds(1, nt - 1), pl.ds(4, 2)], gc_r)

    @pl.when(first)
    def _():
        ab_forward().wait_recv()
        arrived(cd_all, gc_r)

    def gram(j):
        return gall[:, j].reshape(rank, rank).astype(BF16)

    a0, b0, a1, b1, c0, d1 = (gram(j) for j in range(6))

    parts = ((0, 2), (2, 3))

    def keep(j, v):
        v = v.astype(wire)
        sres[j] = v
        res[s, t, j] = v

    def shared(m, k):
        at, size = parts[m]
        span = pl.ds(at, size)
        return copy(sres.at[span], res.at[s, t, span], plane_s, re_r.at[m], 1, ahead(k))

    def onward(m):
        at, size = parts[m]
        blocks = res.at[:, :, pl.ds(at, size)]
        return copy(blocks, blocks, plane_s, fw_r.at[m], 0, t)

    def last(k):
        return copy(sres.at[5], res.at[s, t, 5], plane_s, la_r, 0, ahead(k))

    def share(m):
        for k in range(1, nt):
            shared(m, k).start()

        @pl.when(first)
        def _():
            shared(m, 0).start()

    h0a = mm(h0, a0)
    p1 = p1 + mm(h0, d1)
    s1u0 = v0 + h0a
    s1u1 = v1 + mm(h0, c0)
    base = xh + mm(h0, b0)
    sq1 = sq0 + rowsum(h0f * (v0 + s1u0))
    inv1 = lax.rsqrt(sq1 / width + epsilon)
    pre1 = inv1 * p1
    sig1 = jax.nn.sigmoid(pre1)
    h1 = (pre1 * sig1).astype(BF16)
    h1f = h1.astype(F32)
    keep(0, h0)
    keep(1, h1)
    share(0)
    yu1 = s1u1 + mm(h1, a1)
    yu0 = s1u0 + mm_nt(h1, c0)
    base = base + mm(h1, b1)
    sq2 = sq1 + rowsum(h1f * (s1u1 + yu1))
    inv2 = lax.rsqrt(sq2 / width + epsilon)
    logits = inv2 * base
    expo = jnp.exp(logits - jnp.max(logits, axis=1, keepdims=True))
    cot = expo / rowsum(expo) * validity - onehot
    radial = rowsum(cot * base)
    wh = (inv2 * cot).astype(BF16)
    keep(2, wh)
    ch = inv2 * inv2 * inv2 / width * radial
    hg1 = mm_nt(wh, b1) - ch * yu1
    act1 = hg1 * sig1 * (1.0 + pre1 * (1.0 - sig1))
    w1 = (inv1 * act1).astype(BF16)
    c1 = inv1 * inv1 * inv1 / width * rowsum(act1 * p1)
    ch_h, ch_l = split(ch)
    c1_h, c1_l = split(c1)
    lane = lax.broadcasted_iota(jnp.int32, (own, rank), 1)
    q4 = rank // 4
    keep(3, w1)
    keep(4, jnp.where(
        lane < q4, ch_h.astype(F32),
        jnp.where(lane < 2 * q4, ch_l.astype(F32), jnp.where(lane < 3 * q4, c1_h.astype(F32), c1_l.astype(F32))),
    ))
    share(1)
    hg0 = mm_nt(wh, b0) - ch * yu0 + mm_nt(w1, d1) - c1 * s1u0
    act0 = hg0 * sig0 * (1.0 + pre0 * (1.0 - sig0))
    w0 = (inv0 * act0).astype(BF16)
    keep(5, w0)
    for k in range(1, nt):
        last(k).start()

    @pl.when(s != 0)
    def _():
        last(0).start()

    def got(j):
        return res[:, :, j].reshape(tokens, res.shape[-1])

    def piece(j, full):
        full = full.astype(BF16)
        for i in range(nd):
            sdp[i, j] = full[i * part : (i + 1) * part]

    near_far = far + side * quarter
    deep_far = far + (1 - side) * quarter

    def remote(src, dst, ss, rs, to):
        return pltpu.make_async_remote_copy(
            src_ref=src, dst_ref=dst, send_sem=ss, recv_sem=rs, device_id=(s, to, t), device_id_type=MESH
        )

    def near_copy(k, j):
        to = side * hl + lax.rem(local_d + k, hl)
        return remote(sdp.at[to, j], rnear.at[j, k], dp_s.at[j, k - 1], dp_r.at[j], to)

    def up_copy(i):
        return remote(sdp.at[near_far + i, 1], rfar.at[local_d], far_s.at[i], far_r, near_far + i)

    def relay_copy(g):
        block = pl.ds(near_far if g == 2 else deep_far, quarter)
        return remote(sdp.at[block, 1 if g == 1 else 0], relay.at[g], rel_s.at[g], rel_r.at[g], partner)

    def cross_copy(g, i):
        m = local_d // 2
        to = (near_far if g == 2 else deep_far) + i
        return remote(psum.at[g, i], rcross.at[1 if g == 1 else 0, m], cr_s, cr_r.at[1 if g == 1 else 0], to)

    def small_copy(k):
        to = lax.rem(d + k, nd)
        return remote(spr, rgn.at[d // 2], sm_s, sm_r.at[(to // 2 != d // 2).astype(jnp.int32)], to)

    def small_first():
        return remote(sgn, rsm, su_s, su_r, partner)

    def tail(sec):
        u0, u1 = (oup, up_ref) if sec else (up_ref, oup)

        def collect(m):
            at, size = parts[m]
            span = pl.ds(at, size)
            if sec:
                arrived(block((2 * nt - 1) * size * own_size), re_r.at[m])
                onward(m).start()
            else:
                arrived(res.at[:, :, span], fw_r.at[m])

        def down(state, own_w):
            piece(0, mm_tn(own_w, (state * gain).astype(BF16)))

            @pl.when(outer)
            def _():
                relay_copy(0).start()

            @pl.when(jnp.logical_not(outer))
            def _():
                for k in range(1, hl):
                    near_copy(k, 0).start()

        if sec == 0:
            arrived(block((2 * nt - 1) * own_size), la_r)
            state, own_w = xf, got(5).astype(BF16)
            down(state, own_w)
            for i in range(3):
                sib(i).wait_recv()
        collect(0)
        h0g, h1g = got(0).astype(BF16), got(1).astype(BF16)
        s1 = xf + mm(h0g, u0[...])
        y = s1 + mm(h1g, u1[...])
        collect(1)
        w1g = got(3).astype(BF16)
        if sec:
            state, own_w = s1, w1g
            down(state, own_w)
        cg = got(4).astype(F32)
        chg = cg[:, 0:1] + cg[:, q4 : q4 + 1]
        g = mm_nt(got(2).astype(BF16), head_ref[...]) - chg * y
        if sec == 0:
            c1g = cg[:, 2 * q4 : 2 * q4 + 1] + cg[:, 3 * q4 : 3 * q4 + 1]
            g = g + ogain[...].astype(F32) * mm_nt(w1g, odn[...]) - c1g * s1
        piece(1, mm_tn(h1g if sec else h0g, g.astype(BF16)))
        gain_row = jnp.sum(mm_nt(own_w, dn_ref[...]) * state, axis=0, keepdims=True)
        sgn[0:1, :] = gain_row
        sgn[1:2, :] = jnp.full((1, feats), count, F32)

    @pl.when(first)
    def _():
        tail(0)

    @pl.when(s != 0)
    def _():
        tail(1)

    def end(sec):
        small_first().start()
        queue = [relay_copy(g) for g in range(3)]
        queue += [up_copy(i) for i in range(quarter)]
        queue += [near_copy(k, j) for j in (1, 0) for k in range(1, hl)]
        window = 6 if sec else 3
        for i in range(1, len(queue)):
            if i >= window:
                queue[i - window].wait_send()
            queue[i].start()
        for c in queue[-window:]:
            c.wait_send()
        small_first().wait_send()

    def middle(sec):
        for i in range(quarter):
            up_copy(i).start()
        for k in range(1, hl):
            near_copy(k, 1).start()
        small_first().wait_recv()
        spr[...] = sgn[...] + rsm[...]
        for k in range(1, nd):
            small_copy(k).start()
        for g in range(3):
            relay_copy(g).wait_recv()
            for i in range(quarter):
                at = (near_far if g == 2 else deep_far) + i
                psum[g, i] = (sdp[at, 1 if g == 1 else 0].astype(F32) + relay[g, i].astype(F32)).astype(BF16)
                cross_copy(g, i).start()

    for sec in (0, 1):

        @pl.when(jnp.logical_and(outer, s == sec))
        def _():
            end(sec)

        @pl.when(jnp.logical_and(jnp.logical_not(outer), s == sec))
        def _():
            middle(sec)

    rgn_own = d // 2

    @pl.when(outer)
    def _():
        arrived(rgn.at[rgn_own], sm_r.at[0])
        spr[...] = rgn[rgn_own]

    arrived(rgn.at[pl.ds(1, nd // 2 - 1)], sm_r.at[1])
    small = spr[...]
    for j in range(1, nd // 2):
        p = lax.rem(rgn_own + j, nd // 2)
        small = small + rgn[p]
    out[2 * part : 2 * part + 2, :] = small

    def total(j, from_pairs):
        arrived(rnear.at[j, pl.ds(1, hl - 1)], dp_r.at[j])
        sums = sdp[d, j].astype(F32)
        for k in range(1, hl):
            sums = sums + rnear[j, k].astype(F32)
        if from_pairs:
            arrived(rcross.at[j], cr_r.at[j])
            for m in range(nd // 4):
                sums = sums + rcross[j, m].astype(F32)
        else:
            arrived(rfar, far_r)
            for m in range(hl):
                sums = sums + rfar[m].astype(F32)
        out[j * part : (j + 1) * part, :] = sums

    @pl.when(deep)
    def _():
        total(1, True)

    @pl.when(jnp.logical_not(deep))
    def _():
        total(1, False)

    total(0, True)

    @pl.when(jnp.logical_not(outer))
    def _():
        for i in range(quarter):
            up_copy(i).wait_send()
        sent(psum, cr_s)
        for k in range(1, hl):
            near_copy(k, 1).wait_send()
            near_copy(k, 0).wait_send()
        sent(rgn.at[pl.ds(1, nd - 1)], sm_s)

    common = 2 * rank * feats + tok_size

    @pl.when(first)
    def _():
        sent(block(common + 2 * nt * rows_size + (6 * nt - 1) * own_size), plane_s)

    @pl.when(s != 0)
    def _():
        sib(2).wait_send()
        grams = 10 * (nt - 1) + 6 * nt
        results = 5 * (nt - 1) + nt + 10 * nt
        sent(block(common + 2 * rank * feats + grams * rows_size + results * own_size), plane_s)


def scale_kernel(part, sums, down_out, up_out, gain_out):
    scale = 1.0 / sums[2 * part + 1 : 2 * part + 2, :]
    down_out[...] = sums[0:part, :] * scale
    up_out[...] = sums[part : 2 * part, :] * scale
    gain_out[...] = sums[2 * part : 2 * part + 1, :] * scale


def solution(mesh):
    nt, nd, ns = mesh.shape["tensor"], mesh.shape["dp"], mesh.shape["section"]
    assert ns == 2 and nd % 4 == 0

    def local(inputs, down, up, gains, head, labels, valid):
        micro, per, feats = inputs.shape
        assert micro == ns
        tokens = micro * per
        rank = down.shape[2]
        own, rows, part = tokens // ns // nt, rank // nt, rank // nd
        wire = BF16 if own % 16 == 0 and rows % 16 == 0 else F32
        bulk = (4 * rank + 2 * tokens) * feats + (27 * nt + 16 * nt * rows) * rank * 4 + 64 * nt * own * rank
        bulk = bulk // 2048 + nt * 16 * tokens // 1024
        vmem = pl.BlockSpec(memory_space=pltpu.VMEM)
        dma = pltpu.SemaphoreType.DMA
        anyspace = pl.BlockSpec(memory_space=pl.ANY)
        sums = pl.pallas_call(
            functools.partial(kernel, nt, nd, feats * nt),
            out_shape=pltpu.VMEM((2 * part + 8, feats), F32),
            in_specs=[anyspace] * 7,
            out_specs=vmem,
            scratch_shapes=[
                pltpu.VMEM((tokens, feats), BF16),
                pltpu.VMEM((feats, rank), BF16),
                pltpu.VMEM((rank, feats), BF16),
                pltpu.VMEM((1, feats), BF16),
                pltpu.VMEM((feats, head.shape[1]), BF16),
                pltpu.VMEM((micro, per), jnp.int32),
                pltpu.VMEM((micro, per), jnp.int32),
                pltpu.VMEM((feats, rank), BF16),
                pltpu.VMEM((rank, feats), BF16),
                pltpu.VMEM((1, feats), BF16),
                pltpu.VMEM((2, nt, 3, own, rank), wire),
                pltpu.VMEM((2, nt, 3, own, rank), wire),
                pltpu.VMEM((16, tokens // 2), wire),
                pltpu.VMEM((nt, 16, tokens // 2), wire),
                pltpu.VMEM((nt, 4, rows, rank), wire),
                pltpu.VMEM((2, nt, 4, rows, rank), wire),
                pltpu.VMEM((6, rows, rank), wire),
                pltpu.VMEM((nt, 6, rows, rank), wire),
                pltpu.VMEM((6, own, rank), wire),
                pltpu.VMEM((2, nt, 6, own, rank), wire),
                pltpu.VMEM((nd, 2, part, feats), BF16),
                pltpu.VMEM((2, nd // 2, part, feats), BF16),
                pltpu.VMEM((nd // 2, part, feats), BF16),
                pltpu.VMEM((3, nd // 4, part, feats), BF16),
                pltpu.VMEM((3, nd // 4, part, feats), BF16),
                pltpu.VMEM((2, nd // 4, part, feats), BF16),
                pltpu.VMEM((2, feats), F32),
                pltpu.VMEM((2, feats), F32),
                pltpu.VMEM((2, feats), F32),
                pltpu.VMEM((nd, 2, feats), F32),
                pltpu.VMEM((bulk, 8, 128), F32),
                dma((6,)),
                dma, dma, dma((3,)),
                dma, dma, dma, dma, dma, dma,
                dma((2,)), dma((2,)), dma,
                dma((2, nd // 2 - 1)), dma((2,)),
                dma((nd // 4,)), dma,
                dma((3,)), dma((3,)),
                dma, dma((2,)),
                dma, dma((2,)),
                dma, dma,
            ],
            compiler_params=pltpu.CompilerParams(collective_id=0, has_side_effects=True),
        )(inputs.reshape(tokens, feats), down[0], up[0], gains, head, labels, valid)
        down_t, up_g, gain_g = pl.pallas_call(
            functools.partial(scale_kernel, part),
            out_shape=(
                jax.ShapeDtypeStruct((part, feats), F32),
                jax.ShapeDtypeStruct((part, feats), F32),
                jax.ShapeDtypeStruct((1, feats), F32),
            ),
            in_specs=[vmem],
            out_specs=(vmem,) * 3,
        )(pltpu.with_memory_space_constraint(sums, pltpu.VMEM))
        return down_t.T[None], up_g[None], gain_g

    return jax.shard_map(
        local,
        mesh=mesh,
        in_specs=(
            P(None, "dp", "tensor"),
            P("section", "tensor", None),
            P("section", None, "tensor"),
            P("section", "tensor"),
            P("tensor", None),
            P(None, "dp"),
            P(None, "dp"),
        ),
        out_specs=(
            P("section", "tensor", "dp"),
            P("section", "dp", "tensor"),
            P("section", "tensor"),
        ),
        check_vma=False,
    )
```

```python
import functools

import jax
import jax.numpy as jnp
from jax import lax
from jax.experimental import pallas as pl
from jax.experimental.pallas import tpu as pltpu
from jax.sharding import PartitionSpec as P

MESH = pl.DeviceIdType.MESH
epsilon = 1e-05
F32 = jnp.float32
BF16 = jnp.bfloat16


def mm(a, b):
    return jnp.dot(a, b, preferred_element_type=F32)


def mm_nt(a, b):
    return lax.dot_general(a, b, (((1,), (1,)), ((), ())), preferred_element_type=F32)


def mm_tn(a, b):
    return lax.dot_general(a, b, (((0,), (0,)), ((), ())), preferred_element_type=F32)


def split(v):
    high = v.astype(BF16)
    return high, (v - high.astype(F32)).astype(BF16)


def kernel(
    nt, nd, width,
    x_hbm, dn_hbm, up_hbm, gain_hbm, head_hbm, lab_hbm, val_hbm,
    out,
    x_ref, dn_ref, up_ref, gain_ref, head_ref, lab_ref, val_ref,
    odn, oup, ogain, stok, rtok, ssq, rsq, sgram, rgram, pgram, gall, sres, res,
    sdp, rnear, rfar, relay, psum, rcross, sgn, rsm, spr, rgn,
    bulk, load, plane_s, sib_s, sib_r, tok_r, gr_r, gq_r, ga_r, gf_r, gc_r, re_r, fw_r, la_r, dp_s, dp_r, far_r, rel_r, cr_r, sm_s, sm_r, su_s, su_r,
):
    s, d, t = lax.axis_index("section"), lax.axis_index("dp"), lax.axis_index("tensor")
    first = s == 0
    tokens, feats = x_ref.shape
    rank = dn_ref.shape[1]
    half = tokens // 2
    own = half // nt
    rows = rank // nt
    part = rank // nd
    wire = stok.dtype
    own_size, rows_size = (n * rank * wire.itemsize for n in (own, rows))
    tok_size = (3 * (nt - 1) + 2 * nt) * own_size + (nt - 1) * 16 * half * wire.itemsize

    hl = nd // 2
    quarter = hl // 2
    side = d // hl
    local_d = lax.rem(d, hl)
    far = (1 - side) * hl
    odd = lax.rem(d, 2)
    outer = odd == side
    deep = local_d // quarter == side
    tip = jnp.logical_and(outer, deep)
    partner = d + 1 - 2 * odd

    def ahead(k):
        return lax.rem(t + k, nt)

    def behind(k):
        return lax.rem(t + nt - k, nt)

    loads = [
        pltpu.make_async_copy(a, b, load.at[min(i, 5)])
        for i, (a, b) in enumerate((
            (up_hbm, up_ref), (head_hbm, head_ref), (gain_hbm, gain_ref), (lab_hbm, lab_ref), (val_hbm, val_ref),
            (x_hbm, x_ref), (dn_hbm, dn_ref),
        ))
    ]
    for c in loads:
        c.start()

    barrier = pltpu.get_barrier_semaphore()
    for k in range(1, nd):
        to = lax.rem(d + k, nd)

        @pl.when(jnp.logical_not(jnp.logical_and(tip, to == nd - 1 - d)))
        def _():
            pl.semaphore_signal(barrier, inc=1, device_id=(s, to, t), device_id_type=MESH)

    group = [(k, o) for k in range(nt) for o in (0, 1) if (k, o) != (0, 0)]
    for k, o in group:
        pl.semaphore_signal(barrier, inc=1, device_id=(1 - s if o else s, d, ahead(k)), device_id_type=MESH)

    def copy(src, dst, ss, rs, section, column):
        return pltpu.make_async_remote_copy(
            src_ref=src, dst_ref=dst, send_sem=ss, recv_sem=rs, device_id=(section, d, column), device_id_type=MESH
        )

    def block(size):
        return bulk.at[pl.ds(0, size // (4 * bulk.shape[1] * bulk.shape[2]))]

    def whole(ref, sem):
        return copy(ref, ref, sem, sem, 1 - s, t)

    def arrived(ref, sem):
        whole(ref, sem).wait_recv()

    def sent(ref, sem):
        whole(ref, sem).wait_send()

    def put_gram(j, g):
        g = g.astype(wire)
        for i in range(nt):
            sgram[i, j] = g[i * rows : (i + 1) * rows]

    loads[0].wait()
    up = up_ref[...]
    put_gram(0, mm_nt(up, up))
    loads[1].wait()
    head = head_ref[...]
    put_gram(1, mm(up, head))

    pl.semaphore_wait(barrier, len(group) + nd - 1 - tip.astype(jnp.int32))

    def sib(i):
        a, b = ((up_ref, oup), (dn_ref, odn), (gain_ref, ogain))[i]
        return copy(a, b, sib_s if i == 2 else plane_s, sib_r.at[i], 1 - s, t)

    def ab_scatter(k, sender):
        return copy(
            sgram.at[ahead(k), pl.ds(0, 2)], rgram.at[sender, k, pl.ds(0, 2)], plane_s, gr_r, 1, ahead(k)
        )

    def cd_scatter(k):
        return copy(sgram.at[ahead(k), pl.ds(2, 2)], rgram.at[1, k, pl.ds(2, 2)], plane_s, gq_r, 1, ahead(k))

    def tok_cross(k):
        block = pl.ds(0, 2)
        return copy(
            stok.at[1 - s, ahead(k), block], rtok.at[1, k, block], plane_s, tok_r, 1 - s, ahead(k)
        )

    def tok_own(k):
        return copy(stok.at[s, ahead(k)], rtok.at[0, k], plane_s, tok_r, s, ahead(k))

    def sq_own(k):
        return copy(ssq, rsq.at[k], plane_s, tok_r, s, ahead(k))

    ab_all = gall.at[:, pl.ds(0, 4)]
    cd_all = gall.at[:, pl.ds(4, 2)]

    def ab_gather(k):
        block = pl.ds(0, 4)
        return copy(pgram.at[block], gall.at[t, block], plane_s, ga_r, 1, ahead(k))

    def ab_forward():
        return copy(ab_all, ab_all, plane_s, gf_r, 0, t)

    def cd_gather(k, section):
        block = pl.ds(4, 2)
        return copy(pgram.at[block], gall.at[t, block], plane_s, gc_r, section, ahead(k))

    sib(0).start()
    for k in range(1, nt):
        ab_scatter(k, s).start()

    @pl.when(first)
    def _():
        ab_scatter(0, 0).start()

    for c in loads[2:5]:
        c.wait()
    pltpu.make_async_copy(block(2 * tokens * feats + 2 * rank * feats), block(2 * tokens * feats + 2 * rank * feats), load.at[5]).wait()
    gain = gain_ref[...].astype(F32)
    xb = x_ref[...]
    xf = xb.astype(F32)
    xup = mm_nt(xb, up).astype(wire)
    proj = mm((xf * gain).astype(BF16), dn_ref[...]).astype(wire)
    for b in range(2):
        for i in range(nt):
            at = b * half + i * own
            stok[b, i, 0] = proj[at : at + own]
            stok[b, i, 1] = xup[at : at + own]
    for k in range(nt):
        tok_cross(k).start()

    xm = x_ref[pl.ds(pl.multiple_of(s * half, half), half), :]
    xmf = xm.astype(F32)
    xhead = mm(xm, head).astype(wire)
    for i in range(nt):
        stok[s, i, 2] = xhead[i * own : (i + 1) * own]
    ones = jnp.ones((8, feats), BF16)
    square_h, square_l = split(xmf * xmf)
    row_h, row_l = split(mm_nt(ones, square_h) + mm_nt(ones, square_l))
    ssq[0:8] = row_h.astype(wire)
    ssq[8:16] = row_l.astype(wire)

    @pl.when(s != 0)
    def _():
        sib(0).wait_recv()
        other = oup[...]
        put_gram(2, mm_nt(other, up))
        put_gram(3, mm((other.astype(F32) * gain).astype(BF16), dn_ref[...]))
        for k in range(1, nt):
            cd_scatter(k).start()

    for k in range(1, nt):
        tok_own(k).start()
        sq_own(k).start()

    @pl.when(s != 0)
    def _():
        sib(1).start()
        sib(2).start()
        arrived(block((2 * nt - 1) * 2 * rows_size), gr_r)
        mine1 = sgram[t, 0:2].astype(F32)
        for k in range(1, nt):
            mine1 = mine1 + rgram[1, k, 0:2].astype(F32)
        mine0 = rgram[0, 0, 0:2].astype(F32)
        for k in range(1, nt):
            mine0 = mine0 + rgram[0, k, 0:2].astype(F32)
        for j, v in ((0, mine0.astype(wire)), (2, mine1.astype(wire))):
            pgram[j : j + 2] = v
            gall[t, j : j + 2] = v
        for k in range(1, nt):
            ab_gather(k).start()
        arrived(rgram.at[1, pl.ds(1, nt - 1), pl.ds(2, 2)], gq_r)
        both = sgram[t, 2:4].astype(F32)
        for k in range(1, nt):
            both = both + rgram[1, k, 2:4].astype(F32)
        both = both.astype(wire)
        pgram[4:6] = both
        gall[t, 4:6] = both
        for k in range(1, nt):
            cd_gather(k, 1).start()
        for k in range(nt):
            cd_gather(k, 0).start()

    lab = jnp.where(first, lab_ref[0:1, :], lab_ref[1:2, :])
    val = jnp.where(first, val_ref[0:1, :], val_ref[1:2, :]).astype(F32)
    labels_n = head.shape[1]
    hot_t = jnp.where(lax.broadcasted_iota(jnp.int32, (labels_n, half), 0) == lab, val, 0.0).astype(BF16)
    val_t = jnp.broadcast_to(val, (labels_n, half)).astype(BF16)
    chosen = (
        lax.broadcasted_iota(jnp.int32, (own, half), 0) + t * own
        == lax.broadcasted_iota(jnp.int32, (own, half), 1)
    )
    pick = chosen.astype(F32).astype(BF16)
    onehot = mm_nt(pick, hot_t)
    validity = mm_nt(pick, val_t)
    count = jnp.sum(val_ref[...].astype(F32))

    arrived(block(tok_size), tok_r)
    mine = stok[s, t].astype(F32)
    for k in range(1, nt):
        mine = mine + rtok[0, k].astype(F32)
    theirs = rtok[1, 0, 0:2].astype(F32)
    for k in range(1, nt):
        theirs = theirs + rtok[1, k, 0:2].astype(F32)
    p0 = jnp.where(first, mine[0], theirs[0])
    p1 = jnp.where(first, theirs[0], mine[0])
    v0 = jnp.where(first, mine[1], theirs[1])
    v1 = jnp.where(first, theirs[1], mine[1])
    xh = mine[2]
    sq = ssq[...].astype(F32)
    for k in range(1, nt):
        sq = sq + rsq[k].astype(F32)

    def rowsum(v):
        return jnp.sum(v, axis=1, keepdims=True)

    sq0 = rowsum(jnp.where(chosen, sq[0:1] + sq[8:9], 0.0))
    inv0 = lax.rsqrt(sq0 / width + epsilon)
    pre0 = inv0 * p0
    sig0 = jax.nn.sigmoid(pre0)
    h0 = (pre0 * sig0).astype(BF16)
    h0f = h0.astype(F32)

    @pl.when(s != 0)
    def _():
        arrived(gall.at[pl.ds(1, nt - 1), pl.ds(0, 4)], ga_r)
        ab_forward().start()
        arrived(gall.at[pl.ds(1, nt - 1), pl.ds(4, 2)], gc_r)

    @pl.when(first)
    def _():
        ab_forward().wait_recv()
        arrived(cd_all, gc_r)

    def gram(j):
        return gall[:, j].reshape(rank, rank).astype(BF16)

    a0, b0, a1, b1, c0, d1 = (gram(j) for j in range(6))

    parts = ((0, 2), (2, 3))

    def keep(j, v):
        v = v.astype(wire)
        sres[j] = v
        res[s, t, j] = v

    def shared(m, k):
        at, size = parts[m]
        span = pl.ds(at, size)
        return copy(sres.at[span], res.at[s, t, span], plane_s, re_r.at[m], 1, ahead(k))

    def onward(m):
        at, size = parts[m]
        blocks = res.at[:, :, pl.ds(at, size)]
        return copy(blocks, blocks, plane_s, fw_r.at[m], 0, t)

    def last(k):
        return copy(sres.at[5], res.at[s, t, 5], plane_s, la_r, 0, ahead(k))

    def share(m):
        for k in range(1, nt):
            shared(m, k).start()

        @pl.when(first)
        def _():
            shared(m, 0).start()

    h0a = mm(h0, a0)
    p1 = p1 + mm(h0, d1)
    s1u0 = v0 + h0a
    s1u1 = v1 + mm(h0, c0)
    base = xh + mm(h0, b0)
    sq1 = sq0 + rowsum(h0f * (v0 + s1u0))
    inv1 = lax.rsqrt(sq1 / width + epsilon)
    pre1 = inv1 * p1
    sig1 = jax.nn.sigmoid(pre1)
    h1 = (pre1 * sig1).astype(BF16)
    h1f = h1.astype(F32)
    keep(0, h0)
    keep(1, h1)
    share(0)
    yu1 = s1u1 + mm(h1, a1)
    yu0 = s1u0 + mm_nt(h1, c0)
    base = base + mm(h1, b1)
    sq2 = sq1 + rowsum(h1f * (s1u1 + yu1))
    inv2 = lax.rsqrt(sq2 / width + epsilon)
    logits = inv2 * base
    expo = jnp.exp(logits - jnp.max(logits, axis=1, keepdims=True))
    cot = expo / rowsum(expo) * validity - onehot
    radial = rowsum(cot * base)
    wh = (inv2 * cot).astype(BF16)
    keep(2, wh)
    ch = inv2 * inv2 * inv2 / width * radial
    hg1 = mm_nt(wh, b1) - ch * yu1
    act1 = hg1 * sig1 * (1.0 + pre1 * (1.0 - sig1))
    w1 = (inv1 * act1).astype(BF16)
    c1 = inv1 * inv1 * inv1 / width * rowsum(act1 * p1)
    ch_h, ch_l = split(ch)
    c1_h, c1_l = split(c1)
    lane = lax.broadcasted_iota(jnp.int32, (own, rank), 1)
    q4 = rank // 4
    keep(3, w1)
    keep(4, jnp.where(
        lane < q4, ch_h.astype(F32),
        jnp.where(lane < 2 * q4, ch_l.astype(F32), jnp.where(lane < 3 * q4, c1_h.astype(F32), c1_l.astype(F32))),
    ))
    share(1)
    hg0 = mm_nt(wh, b0) - ch * yu0 + mm_nt(w1, d1) - c1 * s1u0
    act0 = hg0 * sig0 * (1.0 + pre0 * (1.0 - sig0))
    w0 = (inv0 * act0).astype(BF16)
    keep(5, w0)
    for k in range(1, nt):
        last(k).start()

    @pl.when(s != 0)
    def _():
        last(0).start()

    def got(j):
        return res[:, :, j].reshape(tokens, res.shape[-1])

    def piece(j, full):
        full = full.astype(BF16)
        for i in range(nd):
            sdp[i, j] = full[i * part : (i + 1) * part]

    near_far = far + side * quarter
    deep_far = far + (1 - side) * quarter

    def remote(src, dst, ss, rs, to):
        return pltpu.make_async_remote_copy(
            src_ref=src, dst_ref=dst, send_sem=ss, recv_sem=rs, device_id=(s, to, t), device_id_type=MESH
        )

    def near_copy(k, j):
        to = side * hl + lax.rem(local_d + k, hl)
        return remote(sdp.at[to, j], rnear.at[j, k], dp_s, dp_r.at[j], to)

    def up_copy(i):
        return remote(sdp.at[near_far + i, 1], rfar.at[local_d], dp_s, far_r, near_far + i)

    def relay_copy(g):
        block = pl.ds(near_far if g == 2 else deep_far, quarter)
        return remote(sdp.at[block, 1 if g == 1 else 0], relay.at[g], dp_s, rel_r.at[g], partner)

    def cross_copy(g, i):
        m = local_d // 2
        to = (near_far if g == 2 else deep_far) + i
        return remote(psum.at[g, i], rcross.at[1 if g == 1 else 0, m], dp_s, cr_r.at[1 if g == 1 else 0], to)

    def small_copy(k):
        to = lax.rem(d + k, nd)
        return remote(spr, rgn.at[d // 2], sm_s, sm_r.at[(to // 2 != d // 2).astype(jnp.int32)], to)

    def small_first():
        return remote(sgn, rsm, su_s, su_r, partner)

    def tail(sec):
        u0, u1 = (oup, up_ref) if sec else (up_ref, oup)

        def collect(m):
            at, size = parts[m]
            span = pl.ds(at, size)
            if sec:
                arrived(block((2 * nt - 1) * size * own_size), re_r.at[m])
                onward(m).start()
            else:
                arrived(res.at[:, :, span], fw_r.at[m])

        def down(state, own_w):
            piece(0, mm_tn(own_w, (state * gain).astype(BF16)))

            @pl.when(outer)
            def _():
                relay_copy(0).start()

            @pl.when(jnp.logical_not(outer))
            def _():
                for k in range(1, hl):
                    near_copy(k, 0).start()

        if sec == 0:
            arrived(block((2 * nt - 1) * own_size), la_r)
            state, own_w = xf, got(5).astype(BF16)
            down(state, own_w)
            for i in range(3):
                sib(i).wait_recv()
        collect(0)
        h0g, h1g = got(0).astype(BF16), got(1).astype(BF16)
        s1 = xf + mm(h0g, u0[...])
        y = s1 + mm(h1g, u1[...])
        collect(1)
        w1g = got(3).astype(BF16)
        if sec:
            state, own_w = s1, w1g
            down(state, own_w)
        cg = got(4).astype(F32)
        chg = cg[:, 0:1] + cg[:, q4 : q4 + 1]
        g = mm_nt(got(2).astype(BF16), head_ref[...]) - chg * y
        if sec == 0:
            c1g = cg[:, 2 * q4 : 2 * q4 + 1] + cg[:, 3 * q4 : 3 * q4 + 1]
            g = g + ogain[...].astype(F32) * mm_nt(w1g, odn[...]) - c1g * s1
        piece(1, mm_tn(h1g if sec else h0g, g.astype(BF16)))
        gain_row = jnp.sum(mm_nt(own_w, dn_ref[...]) * state, axis=0, keepdims=True)
        sgn[:, 0:feats] = gain_row
        sgn[:, feats:] = jnp.full((1, 128), count, F32)

    @pl.when(first)
    def _():
        tail(0)

    @pl.when(s != 0)
    def _():
        tail(1)

    def end(sec):
        small_first().start()
        queue = [relay_copy(g) for g in (1, 2)]
        queue += [up_copy(i) for i in range(quarter)]
        queue += [near_copy(k, j) for j in (1, 0) for k in range(1, hl)]
        for c in queue:
            c.start()
        small_first().wait_send()

    def middle(sec):
        for i in range(quarter):
            up_copy(i).start()
        for k in range(1, hl):
            near_copy(k, 1).start()
        small_first().wait_recv()
        spr[...] = sgn[...] + rsm[...]
        for k in range(1, nd):
            small_copy(k).start()
        for g in range(3):
            relay_copy(g).wait_recv()
            for i in range(quarter):
                at = (near_far if g == 2 else deep_far) + i
                psum[g, i] = (sdp[at, 1 if g == 1 else 0].astype(F32) + relay[g, i].astype(F32)).astype(BF16)
                cross_copy(g, i).start()

    for sec in (0, 1):

        @pl.when(jnp.logical_and(outer, s == sec))
        def _():
            end(sec)

        @pl.when(jnp.logical_and(jnp.logical_not(outer), s == sec))
        def _():
            middle(sec)

    rgn_own = d // 2

    @pl.when(outer)
    def _():
        arrived(rgn.at[rgn_own], sm_r.at[0])
        spr[...] = rgn[rgn_own]

    arrived(rgn.at[pl.ds(1, nd // 2 - 1)], sm_r.at[1])
    small = spr[...]
    for j in range(1, nd // 2):
        p = lax.rem(rgn_own + j, nd // 2)
        small = small + rgn[p]
    out[2 * part : 2 * part + 1, :] = small[:, 0:feats]
    out[2 * part + 1 : 2 * part + 2, :] = jnp.broadcast_to(small[:, feats : feats + 1], (1, feats))

    def total(j, from_pairs):
        arrived(rnear.at[j, pl.ds(1, hl - 1)], dp_r.at[j])
        sums = sdp[d, j].astype(F32)
        for k in range(1, hl):
            sums = sums + rnear[j, k].astype(F32)
        if from_pairs:
            arrived(rcross.at[j], cr_r.at[j])
            for m in range(nd // 4):
                sums = sums + rcross[j, m].astype(F32)
        else:
            arrived(rfar, far_r)
            for m in range(hl):
                sums = sums + rfar[m].astype(F32)
        out[j * part : (j + 1) * part, :] = sums

    @pl.when(deep)
    def _():
        total(1, True)

    @pl.when(jnp.logical_not(deep))
    def _():
        total(1, False)

    total(0, True)

    @pl.when(jnp.logical_not(outer))
    def _():
        sent(rgn.at[pl.ds(1, nd - 1)], sm_s)

    common = 2 * rank * feats + tok_size
    sent(block((4 * quarter + 2 * (hl - 1)) * 2 * part * feats), dp_s)

    @pl.when(first)
    def _():
        sent(block(common + 2 * nt * rows_size + (6 * nt - 1) * own_size), plane_s)

    @pl.when(s != 0)
    def _():
        sib(2).wait_send()
        grams = 10 * (nt - 1) + 6 * nt
        results = 5 * (nt - 1) + nt + 10 * nt
        sent(block(common + 2 * rank * feats + grams * rows_size + results * own_size), plane_s)


def scale_kernel(part, sums, down_out, up_out, gain_out):
    scale = 1.0 / sums[2 * part + 1 : 2 * part + 2, :]
    down_out[...] = sums[0:part, :] * scale
    up_out[...] = sums[part : 2 * part, :] * scale
    gain_out[...] = sums[2 * part : 2 * part + 1, :] * scale


def solution(mesh):
    nt, nd, ns = mesh.shape["tensor"], mesh.shape["dp"], mesh.shape["section"]
    assert ns == 2 and nd % 4 == 0

    def local(inputs, down, up, gains, head, labels, valid):
        micro, per, feats = inputs.shape
        assert micro == ns
        tokens = micro * per
        rank = down.shape[2]
        own, rows, part = tokens // ns // nt, rank // nt, rank // nd
        wire = BF16 if own % 16 == 0 and rows % 16 == 0 else F32
        bulk = (4 * rank + 2 * tokens) * feats + (27 * nt + 16 * nt * rows) * rank * 4 + 64 * nt * own * rank
        bulk = bulk // 2048 + nt * 16 * tokens // 1024
        vmem = pl.BlockSpec(memory_space=pltpu.VMEM)
        dma = pltpu.SemaphoreType.DMA
        anyspace = pl.BlockSpec(memory_space=pl.ANY)
        sums = pl.pallas_call(
            functools.partial(kernel, nt, nd, feats * nt),
            out_shape=pltpu.VMEM((2 * part + 8, feats), F32),
            in_specs=[anyspace] * 7,
            out_specs=vmem,
            scratch_shapes=[
                pltpu.VMEM((tokens, feats), BF16),
                pltpu.VMEM((feats, rank), BF16),
                pltpu.VMEM((rank, feats), BF16),
                pltpu.VMEM((1, feats), BF16),
                pltpu.VMEM((feats, head.shape[1]), BF16),
                pltpu.VMEM((micro, per), jnp.int32),
                pltpu.VMEM((micro, per), jnp.int32),
                pltpu.VMEM((feats, rank), BF16),
                pltpu.VMEM((rank, feats), BF16),
                pltpu.VMEM((1, feats), BF16),
                pltpu.VMEM((2, nt, 3, own, rank), wire),
                pltpu.VMEM((2, nt, 3, own, rank), wire),
                pltpu.VMEM((16, tokens // 2), wire),
                pltpu.VMEM((nt, 16, tokens // 2), wire),
                pltpu.VMEM((nt, 4, rows, rank), wire),
                pltpu.VMEM((2, nt, 4, rows, rank), wire),
                pltpu.VMEM((6, rows, rank), wire),
                pltpu.VMEM((nt, 6, rows, rank), wire),
                pltpu.VMEM((6, own, rank), wire),
                pltpu.VMEM((2, nt, 6, own, rank), wire),
                pltpu.VMEM((nd, 2, part, feats), BF16),
                pltpu.VMEM((2, nd // 2, part, feats), BF16),
                pltpu.VMEM((nd // 2, part, feats), BF16),
                pltpu.VMEM((3, nd // 4, part, feats), BF16),
                pltpu.VMEM((3, nd // 4, part, feats), BF16),
                pltpu.VMEM((2, nd // 4, part, feats), BF16),
                pltpu.VMEM((1, feats + 128), F32),
                pltpu.VMEM((1, feats + 128), F32),
                pltpu.VMEM((1, feats + 128), F32),
                pltpu.VMEM((nd, 1, feats + 128), F32),
                pltpu.VMEM((bulk, 8, 128), F32),
                dma((6,)),
                dma, dma, dma((3,)),
                dma, dma, dma, dma, dma, dma,
                dma((2,)), dma((2,)), dma,
                dma, dma((2,)), dma, dma((3,)), dma((2,)),
                dma, dma((2,)),
                dma, dma,
            ],
            compiler_params=pltpu.CompilerParams(collective_id=0, has_side_effects=True),
        )(inputs.reshape(tokens, feats), down[0], up[0], gains, head, labels, valid)
        down_t, up_g, gain_g = pl.pallas_call(
            functools.partial(scale_kernel, part),
            out_shape=(
                jax.ShapeDtypeStruct((part, feats), F32),
                jax.ShapeDtypeStruct((part, feats), F32),
                jax.ShapeDtypeStruct((1, feats), F32),
            ),
            in_specs=[vmem],
            out_specs=(vmem,) * 3,
        )(pltpu.with_memory_space_constraint(sums, pltpu.VMEM))
        return down_t.T[None], up_g[None], gain_g

    return jax.shard_map(
        local,
        mesh=mesh,
        in_specs=(
            P(None, "dp", "tensor"),
            P("section", "tensor", None),
            P("section", None, "tensor"),
            P("section", "tensor"),
            P("tensor", None),
            P(None, "dp"),
            P(None, "dp"),
        ),
        out_specs=(
            P("section", "tensor", "dp"),
            P("section", "dp", "tensor"),
            P("section", "tensor"),
        ),
        check_vma=False,
    )
```

```python
import functools

import jax
import jax.numpy as jnp
from jax import lax
from jax.experimental import pallas as pl
from jax.experimental.pallas import tpu as pltpu
from jax.sharding import PartitionSpec as P

MESH = pl.DeviceIdType.MESH
epsilon = 1e-05
F32 = jnp.float32
BF16 = jnp.bfloat16


def mm(a, b):
    return jnp.dot(a, b, preferred_element_type=F32)


def mm_nt(a, b):
    return lax.dot_general(a, b, (((1,), (1,)), ((), ())), preferred_element_type=F32)


def mm_tn(a, b):
    return lax.dot_general(a, b, (((0,), (0,)), ((), ())), preferred_element_type=F32)


def split(v):
    high = v.astype(BF16)
    return high, (v - high.astype(F32)).astype(BF16)


def kernel(
    nt, nd, width,
    x_hbm, dn_hbm, up_hbm, gain_hbm, head_hbm, lab_hbm, val_hbm,
    out,
    x_ref, dn_ref, up_ref, gain_ref, head_ref, lab_ref, val_ref,
    odn, oup, ogain, stok, rtok, ssq, rsq, sgram, rgram, pgram, gall, sres, res,
    sdp, rnear, rfar, relay, psum, rcross, sgn, rsm, spr, rgn,
    bulk, load, plane_s, sib_s, sib_r, tok_r, gr_r, gq_r, ga_r, gf_r, gc_r, re_r, fw_r, la_r, dp_s, dp_r, far_r, rel_r, cr_r, sm_s, sm_r, su_s, su_r,
):
    s, d, t = lax.axis_index("section"), lax.axis_index("dp"), lax.axis_index("tensor")
    first = s == 0
    tokens, feats = x_ref.shape
    rank = dn_ref.shape[1]
    half = tokens // 2
    own = half // nt
    rows = rank // nt
    part = rank // nd
    wire = stok.dtype
    own_size, rows_size = (n * rank * wire.itemsize for n in (own, rows))
    tok_size = (3 * (nt - 1) + 2 * nt) * own_size + (nt - 1) * 16 * half * wire.itemsize

    hl = nd // 2
    quarter = hl // 2
    side = d // hl
    local_d = lax.rem(d, hl)
    far = (1 - side) * hl
    odd = lax.rem(d, 2)
    outer = odd == side
    deep = local_d // quarter == side
    tip = jnp.logical_and(outer, deep)
    partner = d + 1 - 2 * odd

    def ahead(k):
        return lax.rem(t + k, nt)

    def behind(k):
        return lax.rem(t + nt - k, nt)

    loads = [
        pltpu.make_async_copy(a, b, load.at[min(i, 5)])
        for i, (a, b) in enumerate((
            (up_hbm, up_ref), (head_hbm, head_ref), (gain_hbm, gain_ref), (lab_hbm, lab_ref), (val_hbm, val_ref),
            (x_hbm, x_ref), (dn_hbm, dn_ref),
        ))
    ]
    for c in loads:
        c.start()

    barrier = pltpu.get_barrier_semaphore()
    for k in range(1, nd):
        to = lax.rem(d + k, nd)

        @pl.when(jnp.logical_not(jnp.logical_and(tip, to == nd - 1 - d)))
        def _():
            pl.semaphore_signal(barrier, inc=1, device_id=(s, to, t), device_id_type=MESH)

    group = [(k, o) for k in range(nt) for o in (0, 1) if (k, o) != (0, 0)]
    for k, o in group:
        pl.semaphore_signal(barrier, inc=1, device_id=(1 - s if o else s, d, ahead(k)), device_id_type=MESH)

    def copy(src, dst, ss, rs, section, column):
        return pltpu.make_async_remote_copy(
            src_ref=src, dst_ref=dst, send_sem=ss, recv_sem=rs, device_id=(section, d, column), device_id_type=MESH
        )

    def block(size):
        return bulk.at[pl.ds(0, size // (4 * bulk.shape[1] * bulk.shape[2]))]

    def whole(ref, sem):
        return copy(ref, ref, sem, sem, 1 - s, t)

    def arrived(ref, sem):
        whole(ref, sem).wait_recv()

    def sent(ref, sem):
        whole(ref, sem).wait_send()

    def put_gram(j, g):
        g = g.astype(wire)
        for i in range(nt):
            sgram[i, j] = g[i * rows : (i + 1) * rows]

    loads[0].wait()
    up = up_ref[...]
    put_gram(0, mm_nt(up, up))
    loads[1].wait()
    head = head_ref[...]
    put_gram(1, mm(up, head))

    pl.semaphore_wait(barrier, len(group) + nd - 1 - tip.astype(jnp.int32))

    def sib(i):
        a, b = ((up_ref, oup), (dn_ref, odn), (gain_ref, ogain))[i]
        return copy(a, b, sib_s if i == 2 else plane_s, sib_r.at[i], 1 - s, t)

    def ab_scatter(k, sender):
        return copy(
            sgram.at[ahead(k), pl.ds(0, 2)], rgram.at[sender, k, pl.ds(0, 2)], plane_s, gr_r, 1, ahead(k)
        )

    def cd_scatter(k):
        return copy(sgram.at[ahead(k), pl.ds(2, 2)], rgram.at[1, k, pl.ds(2, 2)], plane_s, gq_r, 1, ahead(k))

    def tok_cross(k):
        block = pl.ds(0, 2)
        return copy(
            stok.at[1 - s, ahead(k), block], rtok.at[1, k, block], plane_s, tok_r, 1 - s, ahead(k)
        )

    def tok_own(k):
        return copy(stok.at[s, ahead(k)], rtok.at[0, k], plane_s, tok_r, s, ahead(k))

    def sq_own(k):
        return copy(ssq, rsq.at[k], plane_s, tok_r, s, ahead(k))

    ab_all = gall.at[:, pl.ds(0, 4)]
    cd_all = gall.at[:, pl.ds(4, 2)]

    def ab_gather(k):
        block = pl.ds(0, 4)
        return copy(pgram.at[block], gall.at[t, block], plane_s, ga_r, 1, ahead(k))

    def ab_forward():
        return copy(ab_all, ab_all, plane_s, gf_r, 0, t)

    def cd_gather(k, section):
        block = pl.ds(4, 2)
        return copy(pgram.at[block], gall.at[t, block], plane_s, gc_r, section, ahead(k))

    sib(0).start()
    for k in range(1, nt):
        ab_scatter(k, s).start()

    @pl.when(first)
    def _():
        ab_scatter(0, 0).start()

    for c in loads[2:5]:
        c.wait()
    pltpu.make_async_copy(block(2 * tokens * feats + 2 * rank * feats), block(2 * tokens * feats + 2 * rank * feats), load.at[5]).wait()
    gain = gain_ref[...].astype(F32)
    xb = x_ref[...]
    xf = xb.astype(F32)
    xup = mm_nt(xb, up).astype(wire)
    proj = mm((xf * gain).astype(BF16), dn_ref[...]).astype(wire)
    for b in range(2):
        for i in range(nt):
            at = b * half + i * own
            stok[b, i, 0] = proj[at : at + own]
            stok[b, i, 1] = xup[at : at + own]
    for k in list(range(1, nt)) + [0]:
        tok_cross(k).start()

    xm = x_ref[pl.ds(pl.multiple_of(s * half, half), half), :]
    xmf = xm.astype(F32)
    xhead = mm(xm, head).astype(wire)
    for i in range(nt):
        stok[s, i, 2] = xhead[i * own : (i + 1) * own]
    ones = jnp.ones((8, feats), BF16)
    square_h, square_l = split(xmf * xmf)
    row_h, row_l = split(mm_nt(ones, square_h) + mm_nt(ones, square_l))
    ssq[0:8] = row_h.astype(wire)
    ssq[8:16] = row_l.astype(wire)

    @pl.when(s != 0)
    def _():
        sib(0).wait_recv()
        other = oup[...]
        put_gram(2, mm_nt(other, up))
        put_gram(3, mm((other.astype(F32) * gain).astype(BF16), dn_ref[...]))
        for k in range(1, nt):
            cd_scatter(k).start()

    for k in range(1, nt):
        tok_own(k).start()
        sq_own(k).start()

    @pl.when(s != 0)
    def _():
        sib(1).start()
        sib(2).start()
        arrived(block((2 * nt - 1) * 2 * rows_size), gr_r)
        mine1 = sgram[t, 0:2].astype(F32)
        for k in range(1, nt):
            mine1 = mine1 + rgram[1, k, 0:2].astype(F32)
        mine0 = rgram[0, 0, 0:2].astype(F32)
        for k in range(1, nt):
            mine0 = mine0 + rgram[0, k, 0:2].astype(F32)
        for j, v in ((0, mine0.astype(wire)), (2, mine1.astype(wire))):
            pgram[j : j + 2] = v
            gall[t, j : j + 2] = v
        for k in range(1, nt):
            ab_gather(k).start()
        arrived(rgram.at[1, pl.ds(1, nt - 1), pl.ds(2, 2)], gq_r)
        both = sgram[t, 2:4].astype(F32)
        for k in range(1, nt):
            both = both + rgram[1, k, 2:4].astype(F32)
        both = both.astype(wire)
        pgram[4:6] = both
        gall[t, 4:6] = both
        for k in range(1, nt):
            cd_gather(k, 1).start()
        for k in range(nt):
            cd_gather(k, 0).start()

    lab = jnp.where(first, lab_ref[0:1, :], lab_ref[1:2, :])
    val = jnp.where(first, val_ref[0:1, :], val_ref[1:2, :]).astype(F32)
    labels_n = head.shape[1]
    hot_t = jnp.where(lax.broadcasted_iota(jnp.int32, (labels_n, half), 0) == lab, val, 0.0).astype(BF16)
    val_t = jnp.broadcast_to(val, (labels_n, half)).astype(BF16)
    chosen = (
        lax.broadcasted_iota(jnp.int32, (own, half), 0) + t * own
        == lax.broadcasted_iota(jnp.int32, (own, half), 1)
    )
    pick = chosen.astype(F32).astype(BF16)
    onehot = mm_nt(pick, hot_t)
    validity = mm_nt(pick, val_t)
    count = jnp.sum(val_ref[...].astype(F32))

    arrived(block(tok_size), tok_r)
    mine = stok[s, t].astype(F32)
    for k in range(1, nt):
        mine = mine + rtok[0, k].astype(F32)
    theirs = rtok[1, 0, 0:2].astype(F32)
    for k in range(1, nt):
        theirs = theirs + rtok[1, k, 0:2].astype(F32)
    p0 = jnp.where(first, mine[0], theirs[0])
    p1 = jnp.where(first, theirs[0], mine[0])
    v0 = jnp.where(first, mine[1], theirs[1])
    v1 = jnp.where(first, theirs[1], mine[1])
    xh = mine[2]
    sq = ssq[...].astype(F32)
    for k in range(1, nt):
        sq = sq + rsq[k].astype(F32)

    def rowsum(v):
        return jnp.sum(v, axis=1, keepdims=True)

    sq0 = rowsum(jnp.where(chosen, sq[0:1] + sq[8:9], 0.0))
    inv0 = lax.rsqrt(sq0 / width + epsilon)
    pre0 = inv0 * p0
    sig0 = jax.nn.sigmoid(pre0)
    h0 = (pre0 * sig0).astype(BF16)
    h0f = h0.astype(F32)

    @pl.when(s != 0)
    def _():
        arrived(gall.at[pl.ds(1, nt - 1), pl.ds(0, 4)], ga_r)
        ab_forward().start()
        arrived(gall.at[pl.ds(1, nt - 1), pl.ds(4, 2)], gc_r)

    @pl.when(first)
    def _():
        ab_forward().wait_recv()
        arrived(cd_all, gc_r)

    def gram(j):
        return gall[:, j].reshape(rank, rank).astype(BF16)

    a0, b0, a1, b1, c0, d1 = (gram(j) for j in range(6))

    parts = ((0, 2), (2, 3))

    def keep(j, v):
        v = v.astype(wire)
        sres[j] = v
        res[s, t, j] = v

    def shared(m, k):
        at, size = parts[m]
        span = pl.ds(at, size)
        return copy(sres.at[span], res.at[s, t, span], plane_s, re_r.at[m], 1, ahead(k))

    def onward(m):
        at, size = parts[m]
        blocks = res.at[:, :, pl.ds(at, size)]
        return copy(blocks, blocks, plane_s, fw_r.at[m], 0, t)

    def last(k):
        return copy(sres.at[5], res.at[s, t, 5], plane_s, la_r, 0, ahead(k))

    def share(m):
        for k in range(1, nt):
            shared(m, k).start()

        @pl.when(first)
        def _():
            shared(m, 0).start()

    h0a = mm(h0, a0)
    p1 = p1 + mm(h0, d1)
    s1u0 = v0 + h0a
    s1u1 = v1 + mm(h0, c0)
    base = xh + mm(h0, b0)
    sq1 = sq0 + rowsum(h0f * (v0 + s1u0))
    inv1 = lax.rsqrt(sq1 / width + epsilon)
    pre1 = inv1 * p1
    sig1 = jax.nn.sigmoid(pre1)
    h1 = (pre1 * sig1).astype(BF16)
    h1f = h1.astype(F32)
    keep(0, h0)
    keep(1, h1)
    share(0)
    yu1 = s1u1 + mm(h1, a1)
    yu0 = s1u0 + mm_nt(h1, c0)
    base = base + mm(h1, b1)
    sq2 = sq1 + rowsum(h1f * (s1u1 + yu1))
    inv2 = lax.rsqrt(sq2 / width + epsilon)
    logits = inv2 * base
    expo = jnp.exp(logits - jnp.max(logits, axis=1, keepdims=True))
    cot = expo / rowsum(expo) * validity - onehot
    radial = rowsum(cot * base)
    wh = (inv2 * cot).astype(BF16)
    keep(2, wh)
    ch = inv2 * inv2 * inv2 / width * radial
    hg1 = mm_nt(wh, b1) - ch * yu1
    act1 = hg1 * sig1 * (1.0 + pre1 * (1.0 - sig1))
    w1 = (inv1 * act1).astype(BF16)
    c1 = inv1 * inv1 * inv1 / width * rowsum(act1 * p1)
    ch_h, ch_l = split(ch)
    c1_h, c1_l = split(c1)
    lane = lax.broadcasted_iota(jnp.int32, (own, rank), 1)
    q4 = rank // 4
    keep(3, w1)
    keep(4, jnp.where(
        lane < q4, ch_h.astype(F32),
        jnp.where(lane < 2 * q4, ch_l.astype(F32), jnp.where(lane < 3 * q4, c1_h.astype(F32), c1_l.astype(F32))),
    ))
    share(1)
    hg0 = mm_nt(wh, b0) - ch * yu0 + mm_nt(w1, d1) - c1 * s1u0
    act0 = hg0 * sig0 * (1.0 + pre0 * (1.0 - sig0))
    w0 = (inv0 * act0).astype(BF16)
    keep(5, w0)
    for k in range(1, nt):
        last(k).start()

    @pl.when(s != 0)
    def _():
        last(0).start()

    def got(j):
        return res[:, :, j].reshape(tokens, res.shape[-1])

    def piece(j, full):
        full = full.astype(BF16)
        for i in range(nd):
            sdp[i, j] = full[i * part : (i + 1) * part]

    near_far = far + side * quarter
    deep_far = far + (1 - side) * quarter

    def remote(src, dst, ss, rs, to):
        return pltpu.make_async_remote_copy(
            src_ref=src, dst_ref=dst, send_sem=ss, recv_sem=rs, device_id=(s, to, t), device_id_type=MESH
        )

    def near_copy(k, j):
        to = side * hl + lax.rem(local_d + k, hl)
        return remote(sdp.at[to, j], rnear.at[j, k], dp_s, dp_r.at[j], to)

    def up_copy(i):
        return remote(sdp.at[near_far + i, 1], rfar.at[local_d], dp_s, far_r, near_far + i)

    def relay_copy(g):
        block = pl.ds(near_far if g == 2 else deep_far, quarter)
        return remote(sdp.at[block, 1 if g == 1 else 0], relay.at[g], dp_s, rel_r.at[g], partner)

    def cross_copy(g, i):
        m = local_d // 2
        to = (near_far if g == 2 else deep_far) + i
        return remote(psum.at[g, i], rcross.at[1 if g == 1 else 0, m], dp_s, cr_r.at[1 if g == 1 else 0], to)

    def small_copy(k):
        to = lax.rem(d + k, nd)
        return remote(spr, rgn.at[d // 2], sm_s, sm_r.at[(to // 2 != d // 2).astype(jnp.int32)], to)

    def small_first():
        return remote(sgn, rsm, su_s, su_r, partner)

    def tail(sec):
        u0, u1 = (oup, up_ref) if sec else (up_ref, oup)

        def collect(m):
            at, size = parts[m]
            span = pl.ds(at, size)
            if sec:
                arrived(block((2 * nt - 1) * size * own_size), re_r.at[m])
                onward(m).start()
            else:
                arrived(res.at[:, :, span], fw_r.at[m])

        def down(scaled, own_w):
            piece(0, mm_tn(own_w, scaled))

            @pl.when(outer)
            def _():
                relay_copy(0).start()

            @pl.when(jnp.logical_not(outer))
            def _():
                for k in range(1, hl):
                    near_copy(k, 0).start()

        if sec == 0:
            arrived(block((2 * nt - 1) * own_size), la_r)
            state, own_w = xf, got(5).astype(BF16)
            down((state * gain).astype(BF16), own_w)
            for i in range(3):
                sib(i).wait_recv()
        collect(0)
        h0g, h1g = got(0).astype(BF16), got(1).astype(BF16)
        s1 = xf + mm(h0g, u0[...])
        y = s1 + mm(h1g, u1[...])
        scaled = (s1 * gain).astype(BF16) if sec else None
        collect(1)
        w1g = got(3).astype(BF16)
        if sec:
            state, own_w = s1, w1g
            down(scaled, own_w)
        cg = got(4).astype(F32)
        chg = cg[:, 0:1] + cg[:, q4 : q4 + 1]
        g = mm_nt(got(2).astype(BF16), head_ref[...]) - chg * y
        if sec == 0:
            c1g = cg[:, 2 * q4 : 2 * q4 + 1] + cg[:, 3 * q4 : 3 * q4 + 1]
            g = g + ogain[...].astype(F32) * mm_nt(w1g, odn[...]) - c1g * s1
        piece(1, mm_tn(h1g if sec else h0g, g.astype(BF16)))
        gain_row = jnp.sum(mm_nt(own_w, dn_ref[...]) * state, axis=0, keepdims=True)
        sgn[:, 0:feats] = gain_row
        sgn[:, feats:] = jnp.full((1, 128), count, F32)

    @pl.when(first)
    def _():
        tail(0)

    @pl.when(s != 0)
    def _():
        tail(1)

    def end(sec):
        small_first().start()
        queue = [relay_copy(g) for g in (1, 2)]
        queue = queue[:1] + [up_copy(i) for i in range(quarter)] + queue[1:]
        queue += [near_copy(k, j) for j in (1, 0) for k in range(1, hl)]
        for c in queue:
            c.start()
        small_first().wait_send()

    def middle(sec):
        for i in range(quarter):
            up_copy(i).start()
        for k in range(1, hl):
            near_copy(k, 1).start()
        small_first().wait_recv()
        spr[...] = sgn[...] + rsm[...]
        for k in range(1, nd):
            small_copy(k).start()
        for g in range(3):
            relay_copy(g).wait_recv()
            for i in range(quarter):
                at = (near_far if g == 2 else deep_far) + i
                psum[g, i] = (sdp[at, 1 if g == 1 else 0].astype(F32) + relay[g, i].astype(F32)).astype(BF16)
                cross_copy(g, i).start()

    for sec in (0, 1):

        @pl.when(jnp.logical_and(outer, s == sec))
        def _():
            end(sec)

        @pl.when(jnp.logical_and(jnp.logical_not(outer), s == sec))
        def _():
            middle(sec)

    rgn_own = d // 2

    @pl.when(outer)
    def _():
        arrived(rgn.at[rgn_own], sm_r.at[0])
        spr[...] = rgn[rgn_own]

    arrived(rgn.at[pl.ds(1, nd // 2 - 1)], sm_r.at[1])
    small = spr[...]
    for j in range(1, nd // 2):
        p = lax.rem(rgn_own + j, nd // 2)
        small = small + rgn[p]
    out[2 * part : 2 * part + 1, :] = small[:, 0:feats]
    out[2 * part + 1 : 2 * part + 2, :] = jnp.broadcast_to(small[:, feats : feats + 1], (1, feats))

    def total(j, from_pairs):
        arrived(rnear.at[j, pl.ds(1, hl - 1)], dp_r.at[j])
        sums = sdp[d, j].astype(F32)
        for k in range(1, hl):
            sums = sums + rnear[j, k].astype(F32)
        if from_pairs:
            arrived(rcross.at[j], cr_r.at[j])
            for m in range(nd // 4):
                sums = sums + rcross[j, m].astype(F32)
        else:
            arrived(rfar, far_r)
            for m in range(hl):
                sums = sums + rfar[m].astype(F32)
        out[j * part : (j + 1) * part, :] = sums

    @pl.when(deep)
    def _():
        total(1, True)

    @pl.when(jnp.logical_not(deep))
    def _():
        total(1, False)

    total(0, True)

    @pl.when(jnp.logical_not(outer))
    def _():
        sent(rgn.at[pl.ds(1, nd - 1)], sm_s)

    common = 2 * rank * feats + tok_size
    sent(block((4 * quarter + 2 * (hl - 1)) * 2 * part * feats), dp_s)

    @pl.when(first)
    def _():
        sent(block(common + 2 * nt * rows_size + (6 * nt - 1) * own_size), plane_s)

    @pl.when(s != 0)
    def _():
        sib(2).wait_send()
        grams = 10 * (nt - 1) + 6 * nt
        results = 5 * (nt - 1) + nt + 10 * nt
        sent(block(common + 2 * rank * feats + grams * rows_size + results * own_size), plane_s)


def scale_kernel(part, sums, down_out, up_out, gain_out):
    scale = 1.0 / sums[2 * part + 1 : 2 * part + 2, :]
    down_out[...] = sums[0:part, :] * scale
    up_out[...] = sums[part : 2 * part, :] * scale
    gain_out[...] = sums[2 * part : 2 * part + 1, :] * scale


def solution(mesh):
    nt, nd, ns = mesh.shape["tensor"], mesh.shape["dp"], mesh.shape["section"]
    assert ns == 2 and nd % 4 == 0

    def local(inputs, down, up, gains, head, labels, valid):
        micro, per, feats = inputs.shape
        assert micro == ns
        tokens = micro * per
        rank = down.shape[2]
        own, rows, part = tokens // ns // nt, rank // nt, rank // nd
        wire = BF16 if own % 16 == 0 and rows % 16 == 0 else F32
        bulk = (4 * rank + 2 * tokens) * feats + (27 * nt + 16 * nt * rows) * rank * 4 + 64 * nt * own * rank
        bulk = bulk // 2048 + nt * 16 * tokens // 1024
        vmem = pl.BlockSpec(memory_space=pltpu.VMEM)
        dma = pltpu.SemaphoreType.DMA
        anyspace = pl.BlockSpec(memory_space=pl.ANY)
        sums = pl.pallas_call(
            functools.partial(kernel, nt, nd, feats * nt),
            out_shape=pltpu.VMEM((2 * part + 8, feats), F32),
            in_specs=[anyspace] * 7,
            out_specs=vmem,
            scratch_shapes=[
                pltpu.VMEM((tokens, feats), BF16),
                pltpu.VMEM((feats, rank), BF16),
                pltpu.VMEM((rank, feats), BF16),
                pltpu.VMEM((1, feats), BF16),
                pltpu.VMEM((feats, head.shape[1]), BF16),
                pltpu.VMEM((micro, per), jnp.int32),
                pltpu.VMEM((micro, per), jnp.int32),
                pltpu.VMEM((feats, rank), BF16),
                pltpu.VMEM((rank, feats), BF16),
                pltpu.VMEM((1, feats), BF16),
                pltpu.VMEM((2, nt, 3, own, rank), wire),
                pltpu.VMEM((2, nt, 3, own, rank), wire),
                pltpu.VMEM((16, tokens // 2), wire),
                pltpu.VMEM((nt, 16, tokens // 2), wire),
                pltpu.VMEM((nt, 4, rows, rank), wire),
                pltpu.VMEM((2, nt, 4, rows, rank), wire),
                pltpu.VMEM((6, rows, rank), wire),
                pltpu.VMEM((nt, 6, rows, rank), wire),
                pltpu.VMEM((6, own, rank), wire),
                pltpu.VMEM((2, nt, 6, own, rank), wire),
                pltpu.VMEM((nd, 2, part, feats), BF16),
                pltpu.VMEM((2, nd // 2, part, feats), BF16),
                pltpu.VMEM((nd // 2, part, feats), BF16),
                pltpu.VMEM((3, nd // 4, part, feats), BF16),
                pltpu.VMEM((3, nd // 4, part, feats), BF16),
                pltpu.VMEM((2, nd // 4, part, feats), BF16),
                pltpu.VMEM((1, feats + 128), F32),
                pltpu.VMEM((1, feats + 128), F32),
                pltpu.VMEM((1, feats + 128), F32),
                pltpu.VMEM((nd, 1, feats + 128), F32),
                pltpu.VMEM((bulk, 8, 128), F32),
                dma((6,)),
                dma, dma, dma((3,)),
                dma, dma, dma, dma, dma, dma,
                dma((2,)), dma((2,)), dma,
                dma, dma((2,)), dma, dma((3,)), dma((2,)),
                dma, dma((2,)),
                dma, dma,
            ],
            compiler_params=pltpu.CompilerParams(collective_id=0, has_side_effects=True),
        )(inputs.reshape(tokens, feats), down[0], up[0], gains, head, labels, valid)
        down_t, up_g, gain_g = pl.pallas_call(
            functools.partial(scale_kernel, part),
            out_shape=(
                jax.ShapeDtypeStruct((part, feats), F32),
                jax.ShapeDtypeStruct((part, feats), F32),
                jax.ShapeDtypeStruct((1, feats), F32),
            ),
            in_specs=[vmem],
            out_specs=(vmem,) * 3,
        )(pltpu.with_memory_space_constraint(sums, pltpu.VMEM))
        return down_t.T[None], up_g[None], gain_g

    return jax.shard_map(
        local,
        mesh=mesh,
        in_specs=(
            P(None, "dp", "tensor"),
            P("section", "tensor", None),
            P("section", None, "tensor"),
            P("section", "tensor"),
            P("tensor", None),
            P(None, "dp"),
            P(None, "dp"),
        ),
        out_specs=(
            P("section", "tensor", "dp"),
            P("section", "dp", "tensor"),
            P("section", "tensor"),
        ),
        check_vma=False,
    )
```

```python
import functools

import jax
import jax.numpy as jnp
from jax import lax
from jax.experimental import pallas as pl
from jax.experimental.pallas import tpu as pltpu
from jax.sharding import PartitionSpec as P

MESH = pl.DeviceIdType.MESH
epsilon = 1e-05
F32 = jnp.float32
BF16 = jnp.bfloat16


def mm(a, b):
    return jnp.dot(a, b, preferred_element_type=F32)


def mm_nt(a, b):
    return lax.dot_general(a, b, (((1,), (1,)), ((), ())), preferred_element_type=F32)


def mm_tn(a, b):
    return lax.dot_general(a, b, (((0,), (0,)), ((), ())), preferred_element_type=F32)


def split(v):
    high = v.astype(BF16)
    return high, (v - high.astype(F32)).astype(BF16)


def kernel(
    nt, nd, width,
    x_hbm, dn_hbm, up_hbm, gain_hbm, head_hbm, lab_hbm, val_hbm,
    out,
    x_ref, dn_ref, up_ref, gain_ref, head_ref, lab_ref, val_ref,
    odn, oup, ogain, stok, rtok, ssq, rsq, sgram, rgram, pgram, gall, sres, res,
    sdp, rnear, rfar, relay, psum, rcross, sgn, rsm, spr, rgn,
    bulk, load, plane_s, sib_s, sib_r, tok_r, gr_r, gq_r, ga_r, gc_r, re_r, fw_r, la_r, dp_s, dp_r, far_r, rel_r, cr_r, sm_s, sm_r, su_r,
):
    s, d, t = lax.axis_index("section"), lax.axis_index("dp"), lax.axis_index("tensor")
    first = s == 0
    tokens, feats = x_ref.shape
    rank = dn_ref.shape[1]
    half = tokens // 2
    own = half // nt
    rows = rank // nt
    part = rank // nd
    wire = stok.dtype
    own_size, rows_size = (n * rank * wire.itemsize for n in (own, rows))
    tok_size = (3 * (nt - 1) + 2 * nt) * own_size + (nt - 1) * 16 * half * wire.itemsize

    hl = nd // 2
    quarter = hl // 2
    side = d // hl
    local_d = lax.rem(d, hl)
    far = (1 - side) * hl
    odd = lax.rem(d, 2)
    outer = odd == side
    deep = local_d // quarter == side
    tip = jnp.logical_and(outer, deep)
    partner = d + 1 - 2 * odd

    def ahead(k):
        return lax.rem(t + k, nt)

    def behind(k):
        return lax.rem(t + nt - k, nt)

    loads = [
        pltpu.make_async_copy(a, b, load.at[min(i, 5)])
        for i, (a, b) in enumerate((
            (up_hbm, up_ref), (head_hbm, head_ref), (gain_hbm, gain_ref), (lab_hbm, lab_ref), (val_hbm, val_ref),
            (x_hbm, x_ref), (dn_hbm, dn_ref),
        ))
    ]
    loads[0].start()

    barrier = pltpu.get_barrier_semaphore()
    for k in range(1, nd):
        to = lax.rem(d + k, nd)

        @pl.when(jnp.logical_not(jnp.logical_and(tip, to == nd - 1 - d)))
        def _():
            pl.semaphore_signal(barrier, inc=1, device_id=(s, to, t), device_id_type=MESH)

    group = [(k, o) for k in range(nt) for o in (0, 1) if (k, o) != (0, 0)]
    for k, o in group:
        pl.semaphore_signal(barrier, inc=1, device_id=(1 - s if o else s, d, ahead(k)), device_id_type=MESH)

    for c in loads[1:]:
        c.start()

    def copy(src, dst, ss, rs, section, column):
        return pltpu.make_async_remote_copy(
            src_ref=src, dst_ref=dst, send_sem=ss, recv_sem=rs, device_id=(section, d, column), device_id_type=MESH
        )

    def block(size):
        return bulk.at[pl.ds(0, size // (4 * bulk.shape[1] * bulk.shape[2]))]

    def whole(ref, sem):
        return copy(ref, ref, sem, sem, 1 - s, t)

    def arrived(ref, sem):
        whole(ref, sem).wait_recv()

    def sent(ref, sem):
        whole(ref, sem).wait_send()

    def put_gram(j, g):
        g = g.astype(wire)
        for i in range(nt):
            sgram[i, j] = g[i * rows : (i + 1) * rows]

    loads[0].wait()
    up = up_ref[...]
    put_gram(0, mm_nt(up, up))
    loads[1].wait()
    head = head_ref[...]
    put_gram(1, mm(up, head))

    pl.semaphore_wait(barrier, len(group) + nd - 1 - tip.astype(jnp.int32))

    def sib(i):
        a, b = ((up_ref, oup), (dn_ref, odn), (gain_ref, ogain))[i]
        return copy(a, b, sib_s if i == 2 else plane_s, sib_r.at[i // 2], 1 - s, t)

    def ab_scatter(k, sender):
        return copy(
            sgram.at[ahead(k), pl.ds(0, 2)], rgram.at[sender, k, pl.ds(0, 2)], plane_s, gr_r, 1, ahead(k)
        )

    def cd_scatter(k):
        return copy(sgram.at[ahead(k), pl.ds(2, 2)], rgram.at[1, k, pl.ds(2, 2)], plane_s, gq_r, 1, ahead(k))

    def tok_cross(k):
        block = pl.ds(0, 2)
        return copy(
            stok.at[1 - s, ahead(k), block], rtok.at[1, k, block], plane_s, tok_r, 1 - s, ahead(k)
        )

    def tok_own(k):
        return copy(stok.at[s, ahead(k)], rtok.at[0, k], plane_s, tok_r, s, ahead(k))

    def sq_own(k):
        return copy(ssq, rsq.at[k], plane_s, tok_r, s, ahead(k))

    ab_all = gall.at[:, pl.ds(0, 4)]
    cd_all = gall.at[:, pl.ds(4, 2)]

    def ab_gather(k):
        block = pl.ds(0, 4)
        return copy(pgram.at[block], gall.at[t, block], plane_s, ga_r, 1, ahead(k))

    def ab_forward():
        return copy(ab_all, ab_all, plane_s, gc_r, 0, t)

    def cd_gather(k, section):
        block = pl.ds(4, 2)
        return copy(pgram.at[block], gall.at[t, block], plane_s, gc_r, section, ahead(k))

    sib(0).start()
    for k in range(1, nt):
        ab_scatter(k, s).start()

    @pl.when(first)
    def _():
        ab_scatter(0, 0).start()

    for c in loads[2:5]:
        c.wait()
    pltpu.make_async_copy(block(2 * tokens * feats + 2 * rank * feats), block(2 * tokens * feats + 2 * rank * feats), load.at[5]).wait()
    gain = gain_ref[...].astype(F32)
    xb = x_ref[...]
    xf = xb.astype(F32)
    xup = mm_nt(xb, up).astype(wire)
    proj = mm((xf * gain).astype(BF16), dn_ref[...]).astype(wire)
    for b in range(2):
        for i in range(nt):
            at = b * half + i * own
            stok[b, i, 0] = proj[at : at + own]
            stok[b, i, 1] = xup[at : at + own]
    for k in list(range(1, nt)) + [0]:
        tok_cross(k).start()

    xm = x_ref[pl.ds(pl.multiple_of(s * half, half), half), :]
    xmf = xm.astype(F32)
    xhead = mm(xm, head).astype(wire)
    for i in range(nt):
        stok[s, i, 2] = xhead[i * own : (i + 1) * own]
    ones = jnp.ones((8, feats), BF16)
    square_h, square_l = split(xmf * xmf)
    row_h, row_l = split(mm_nt(ones, square_h) + mm_nt(ones, square_l))
    ssq[0:8] = row_h.astype(wire)
    ssq[8:16] = row_l.astype(wire)

    @pl.when(s != 0)
    def _():
        sib(0).wait_recv()
        other = oup[...]
        put_gram(2, mm_nt(other, up))
        put_gram(3, mm((other.astype(F32) * gain).astype(BF16), dn_ref[...]))
        for k in range(1, nt):
            cd_scatter(k).start()

    for k in range(1, nt):
        tok_own(k).start()
        sq_own(k).start()

    @pl.when(s != 0)
    def _():
        sib(1).start()
        sib(2).start()
        arrived(block((2 * nt - 1) * 2 * rows_size), gr_r)
        mine1 = sgram[t, 0:2].astype(F32)
        for k in range(1, nt):
            mine1 = mine1 + rgram[1, k, 0:2].astype(F32)
        mine0 = rgram[0, 0, 0:2].astype(F32)
        for k in range(1, nt):
            mine0 = mine0 + rgram[0, k, 0:2].astype(F32)
        for j, v in ((0, mine0.astype(wire)), (2, mine1.astype(wire))):
            pgram[j : j + 2] = v
            gall[t, j : j + 2] = v
        for k in range(1, nt):
            ab_gather(k).start()
        arrived(rgram.at[1, pl.ds(1, nt - 1), pl.ds(2, 2)], gq_r)
        both = sgram[t, 2:4].astype(F32)
        for k in range(1, nt):
            both = both + rgram[1, k, 2:4].astype(F32)
        both = both.astype(wire)
        pgram[4:6] = both
        gall[t, 4:6] = both
        for k in range(1, nt):
            cd_gather(k, 1).start()
        for k in range(nt):
            cd_gather(k, 0).start()

    lab = jnp.where(first, lab_ref[0:1, :], lab_ref[1:2, :])
    val = jnp.where(first, val_ref[0:1, :], val_ref[1:2, :]).astype(F32)
    labels_n = head.shape[1]
    hot_t = jnp.where(lax.broadcasted_iota(jnp.int32, (labels_n, half), 0) == lab, val, 0.0).astype(BF16)
    val_t = jnp.broadcast_to(val, (labels_n, half)).astype(BF16)
    chosen = (
        lax.broadcasted_iota(jnp.int32, (own, half), 0) + t * own
        == lax.broadcasted_iota(jnp.int32, (own, half), 1)
    )
    pick = chosen.astype(F32).astype(BF16)
    onehot = mm_nt(pick, hot_t)
    validity = mm_nt(pick, val_t)
    count = jnp.sum(val_ref[...].astype(F32))

    arrived(block(tok_size), tok_r)
    mine = stok[s, t].astype(F32)
    for k in range(1, nt):
        mine = mine + rtok[0, k].astype(F32)
    theirs = rtok[1, 0, 0:2].astype(F32)
    for k in range(1, nt):
        theirs = theirs + rtok[1, k, 0:2].astype(F32)
    p0 = jnp.where(first, mine[0], theirs[0])
    p1 = jnp.where(first, theirs[0], mine[0])
    v0 = jnp.where(first, mine[1], theirs[1])
    v1 = jnp.where(first, theirs[1], mine[1])
    xh = mine[2]
    sq = ssq[...].astype(F32)
    for k in range(1, nt):
        sq = sq + rsq[k].astype(F32)

    def rowsum(v):
        return jnp.sum(v, axis=1, keepdims=True)

    sq0 = rowsum(jnp.where(chosen, sq[0:1] + sq[8:9], 0.0))
    inv0 = lax.rsqrt(sq0 / width + epsilon)
    pre0 = inv0 * p0
    sig0 = jax.nn.sigmoid(pre0)
    h0 = (pre0 * sig0).astype(BF16)
    h0f = h0.astype(F32)

    @pl.when(s != 0)
    def _():
        arrived(gall.at[pl.ds(1, nt - 1), pl.ds(0, 4)], ga_r)
        ab_forward().start()
        arrived(gall.at[pl.ds(1, nt - 1), pl.ds(4, 2)], gc_r)

    @pl.when(first)
    def _():
        arrived(block(6 * nt * rows_size), gc_r)

    def gram(j):
        return gall[:, j].reshape(rank, rank).astype(BF16)

    a0, b0, a1, b1, c0, d1 = (gram(j) for j in range(6))

    parts = ((0, 2), (2, 3))

    def keep(j, v):
        v = v.astype(wire)
        sres[j] = v
        res[s, t, j] = v

    def shared(m, k):
        at, size = parts[m]
        span = pl.ds(at, size)
        return copy(sres.at[span], res.at[s, t, span], plane_s, re_r.at[m], 1, ahead(k))

    def onward(m):
        at, size = parts[m]
        blocks = res.at[:, :, pl.ds(at, size)]
        return copy(blocks, blocks, plane_s, fw_r.at[m], 0, t)

    def last(k):
        return copy(sres.at[5], res.at[s, t, 5], plane_s, la_r, 0, ahead(k))

    def share(m):
        for k in range(1, nt):
            shared(m, k).start()

        @pl.when(first)
        def _():
            shared(m, 0).start()

    h0a = mm(h0, a0)
    p1 = p1 + mm(h0, d1)
    s1u0 = v0 + h0a
    s1u1 = v1 + mm(h0, c0)
    base = xh + mm(h0, b0)
    sq1 = sq0 + rowsum(h0f * (v0 + s1u0))
    inv1 = lax.rsqrt(sq1 / width + epsilon)
    pre1 = inv1 * p1
    sig1 = jax.nn.sigmoid(pre1)
    h1 = (pre1 * sig1).astype(BF16)
    h1f = h1.astype(F32)
    keep(0, h0)
    keep(1, h1)
    share(0)
    yu1 = s1u1 + mm(h1, a1)
    yu0 = s1u0 + mm_nt(h1, c0)
    base = base + mm(h1, b1)
    sq2 = sq1 + rowsum(h1f * (s1u1 + yu1))
    inv2 = lax.rsqrt(sq2 / width + epsilon)
    logits = inv2 * base
    expo = jnp.exp(logits - jnp.max(logits, axis=1, keepdims=True))
    cot = expo / rowsum(expo) * validity - onehot
    radial = rowsum(cot * base)
    wh = (inv2 * cot).astype(BF16)
    keep(2, wh)
    ch = inv2 * inv2 * inv2 / width * radial
    hg1 = mm_nt(wh, b1) - ch * yu1
    act1 = hg1 * sig1 * (1.0 + pre1 * (1.0 - sig1))
    w1 = (inv1 * act1).astype(BF16)
    c1 = inv1 * inv1 * inv1 / width * rowsum(act1 * p1)
    ch_h, ch_l = split(ch)
    c1_h, c1_l = split(c1)
    lane = lax.broadcasted_iota(jnp.int32, (own, rank), 1)
    q4 = rank // 4
    keep(3, w1)
    keep(4, jnp.where(
        lane < q4, ch_h.astype(F32),
        jnp.where(lane < 2 * q4, ch_l.astype(F32), jnp.where(lane < 3 * q4, c1_h.astype(F32), c1_l.astype(F32))),
    ))
    share(1)
    hg0 = mm_nt(wh, b0) - ch * yu0 + mm_nt(w1, d1) - c1 * s1u0
    act0 = hg0 * sig0 * (1.0 + pre0 * (1.0 - sig0))
    w0 = (inv0 * act0).astype(BF16)
    keep(5, w0)
    for k in range(1, nt):
        last(k).start()

    @pl.when(s != 0)
    def _():
        last(0).start()

    def got(j):
        return res[:, :, j].reshape(tokens, res.shape[-1])

    def piece(j, full):
        full = full.astype(BF16)
        for i in range(nd):
            sdp[i, j] = full[i * part : (i + 1) * part]

    near_far = far + side * quarter
    deep_far = far + (1 - side) * quarter

    def remote(src, dst, ss, rs, to):
        return pltpu.make_async_remote_copy(
            src_ref=src, dst_ref=dst, send_sem=ss, recv_sem=rs, device_id=(s, to, t), device_id_type=MESH
        )

    def near_copy(k, j):
        to = side * hl + lax.rem(local_d + k, hl)
        return remote(sdp.at[to, j], rnear.at[j, k], dp_s, dp_r.at[j], to)

    def up_copy(i):
        return remote(sdp.at[near_far + i, 1], rfar.at[local_d], dp_s, far_r, near_far + i)

    def relay_copy(g):
        block = pl.ds(near_far if g == 2 else deep_far, quarter)
        return remote(sdp.at[block, 1 if g == 1 else 0], relay.at[g], dp_s, rel_r.at[g], partner)

    def cross_copy(g, i):
        m = local_d // 2
        to = (near_far if g == 2 else deep_far) + i
        return remote(psum.at[g, i], rcross.at[1 if g == 1 else 0, m], dp_s, cr_r.at[1 if g == 1 else 0], to)

    def small_copy(k):
        to = lax.rem(d + k, nd)
        return remote(spr, rgn.at[d // 2], sm_s, sm_r.at[(to // 2 != d // 2).astype(jnp.int32)], to)

    def small_first():
        return remote(sgn, rsm, sm_s, su_r, partner)

    def tail(sec):
        u0, u1 = (oup, up_ref) if sec else (up_ref, oup)

        def collect(m):
            at, size = parts[m]
            span = pl.ds(at, size)
            if sec:
                arrived(block((2 * nt - 1) * size * own_size), re_r.at[m])
                onward(m).start()
            else:
                arrived(res.at[:, :, span], fw_r.at[m])

        def down(scaled, own_w):
            piece(0, mm_tn(own_w, scaled))

            @pl.when(outer)
            def _():
                relay_copy(0).start()

            @pl.when(jnp.logical_not(outer))
            def _():
                for k in range(1, hl):
                    near_copy(k, 0).start()

        if sec == 0:
            arrived(block((2 * nt - 1) * own_size), la_r)
            state, own_w = xf, got(5).astype(BF16)
            down((state * gain).astype(BF16), own_w)
            arrived(block(4 * rank * feats), sib_r.at[0])
            sib(2).wait_recv()
        collect(0)
        h0g, h1g = got(0).astype(BF16), got(1).astype(BF16)
        s1 = xf + mm(h0g, u0[...])
        y = s1 + mm(h1g, u1[...])
        scaled = (s1 * gain).astype(BF16) if sec else None
        collect(1)
        w1g = got(3).astype(BF16)
        if sec:
            state, own_w = s1, w1g
            down(scaled, own_w)
        cg = got(4).astype(F32)
        chg = cg[:, 0:1] + cg[:, q4 : q4 + 1]
        g = mm_nt(got(2).astype(BF16), head_ref[...]) - chg * y
        if sec == 0:
            c1g = cg[:, 2 * q4 : 2 * q4 + 1] + cg[:, 3 * q4 : 3 * q4 + 1]
            g = g + ogain[...].astype(F32) * mm_nt(w1g, odn[...]) - c1g * s1
        piece(1, mm_tn(h1g if sec else h0g, g.astype(BF16)))
        gain_row = jnp.sum(mm_nt(own_w, dn_ref[...]) * state, axis=0, keepdims=True)
        sgn[:, 0:feats] = gain_row
        sgn[:, feats:] = jnp.full((1, 128), count, F32)

    @pl.when(first)
    def _():
        tail(0)

    @pl.when(s != 0)
    def _():
        tail(1)

    def end(sec):
        small_first().start()
        queue = [relay_copy(g) for g in (1, 2)]
        queue = queue[:1] + [up_copy(i) for i in range(quarter)] + queue[1:]
        queue += [near_copy(k, j) for j in (1, 0) for k in range(1, hl)]
        for c in queue:
            c.start()
        small_first().wait_send()

    def middle(sec):
        for i in range(quarter):
            up_copy(i).start()
        for k in range(1, hl):
            near_copy(k, 1).start()
        small_first().wait_recv()
        spr[...] = sgn[...] + rsm[...]
        for k in range(1, nd):
            small_copy(k).start()
        for g in range(3):
            relay_copy(g).wait_recv()
            for i in range(quarter):
                at = (near_far if g == 2 else deep_far) + i
                psum[g, i] = (sdp[at, 1 if g == 1 else 0].astype(F32) + relay[g, i].astype(F32)).astype(BF16)
                cross_copy(g, i).start()

    for sec in (0, 1):

        @pl.when(jnp.logical_and(outer, s == sec))
        def _():
            end(sec)

        @pl.when(jnp.logical_and(jnp.logical_not(outer), s == sec))
        def _():
            middle(sec)

    rgn_own = d // 2

    @pl.when(outer)
    def _():
        arrived(rgn.at[rgn_own], sm_r.at[0])
        spr[...] = rgn[rgn_own]

    arrived(rgn.at[pl.ds(1, nd // 2 - 1)], sm_r.at[1])
    small = spr[...]
    for j in range(1, nd // 2):
        p = lax.rem(rgn_own + j, nd // 2)
        small = small + rgn[p]
    out[2 * part : 2 * part + 1, :] = small[:, 0:feats]
    out[2 * part + 1 : 2 * part + 2, :] = jnp.broadcast_to(small[:, feats : feats + 1], (1, feats))

    def total(j, from_pairs):
        arrived(rnear.at[j, pl.ds(1, hl - 1)], dp_r.at[j])
        sums = sdp[d, j].astype(F32)
        for k in range(1, hl):
            sums = sums + rnear[j, k].astype(F32)
        if from_pairs:
            arrived(rcross.at[j], cr_r.at[j])
            for m in range(nd // 4):
                sums = sums + rcross[j, m].astype(F32)
        else:
            arrived(rfar, far_r)
            for m in range(hl):
                sums = sums + rfar[m].astype(F32)
        out[j * part : (j + 1) * part, :] = sums

    @pl.when(deep)
    def _():
        total(1, True)

    @pl.when(jnp.logical_not(deep))
    def _():
        total(1, False)

    total(0, True)

    @pl.when(jnp.logical_not(outer))
    def _():
        sent(rgn.at[pl.ds(1, nd - 1)], sm_s)

    common = 2 * rank * feats + tok_size
    sent(block((4 * quarter + 2 * (hl - 1)) * 2 * part * feats), dp_s)

    @pl.when(first)
    def _():
        sent(block(common + 2 * nt * rows_size + (6 * nt - 1) * own_size), plane_s)

    @pl.when(s != 0)
    def _():
        sib(2).wait_send()
        grams = 10 * (nt - 1) + 6 * nt
        results = 5 * (nt - 1) + nt + 10 * nt
        sent(block(common + 2 * rank * feats + grams * rows_size + results * own_size), plane_s)


def scale_kernel(part, sums, down_out, up_out, gain_out):
    scale = 1.0 / sums[2 * part + 1 : 2 * part + 2, :]
    down_out[...] = sums[0:part, :] * scale
    up_out[...] = sums[part : 2 * part, :] * scale
    gain_out[...] = sums[2 * part : 2 * part + 1, :] * scale


def solution(mesh):
    nt, nd, ns = mesh.shape["tensor"], mesh.shape["dp"], mesh.shape["section"]
    assert ns == 2 and nd % 4 == 0

    def local(inputs, down, up, gains, head, labels, valid):
        micro, per, feats = inputs.shape
        assert micro == ns
        tokens = micro * per
        rank = down.shape[2]
        own, rows, part = tokens // ns // nt, rank // nt, rank // nd
        wire = BF16 if own % 16 == 0 and rows % 16 == 0 else F32
        bulk = (4 * rank + 2 * tokens) * feats + (27 * nt + 16 * nt * rows) * rank * 4 + 64 * nt * own * rank
        bulk = bulk // 2048 + nt * 16 * tokens // 1024
        vmem = pl.BlockSpec(memory_space=pltpu.VMEM)
        dma = pltpu.SemaphoreType.DMA
        anyspace = pl.BlockSpec(memory_space=pl.ANY)
        sums = pl.pallas_call(
            functools.partial(kernel, nt, nd, feats * nt),
            out_shape=pltpu.VMEM((2 * part + 8, feats), F32),
            in_specs=[anyspace] * 7,
            out_specs=vmem,
            scratch_shapes=[
                pltpu.VMEM((tokens, feats), BF16),
                pltpu.VMEM((feats, rank), BF16),
                pltpu.VMEM((rank, feats), BF16),
                pltpu.VMEM((1, feats), BF16),
                pltpu.VMEM((feats, head.shape[1]), BF16),
                pltpu.VMEM((micro, per), jnp.int32),
                pltpu.VMEM((micro, per), jnp.int32),
                pltpu.VMEM((feats, rank), BF16),
                pltpu.VMEM((rank, feats), BF16),
                pltpu.VMEM((1, feats), BF16),
                pltpu.VMEM((2, nt, 3, own, rank), wire),
                pltpu.VMEM((2, nt, 3, own, rank), wire),
                pltpu.VMEM((16, tokens // 2), wire),
                pltpu.VMEM((nt, 16, tokens // 2), wire),
                pltpu.VMEM((nt, 4, rows, rank), wire),
                pltpu.VMEM((2, nt, 4, rows, rank), wire),
                pltpu.VMEM((6, rows, rank), wire),
                pltpu.VMEM((nt, 6, rows, rank), wire),
                pltpu.VMEM((6, own, rank), wire),
                pltpu.VMEM((2, nt, 6, own, rank), wire),
                pltpu.VMEM((nd, 2, part, feats), BF16),
                pltpu.VMEM((2, nd // 2, part, feats), BF16),
                pltpu.VMEM((nd // 2, part, feats), BF16),
                pltpu.VMEM((3, nd // 4, part, feats), BF16),
                pltpu.VMEM((3, nd // 4, part, feats), BF16),
                pltpu.VMEM((2, nd // 4, part, feats), BF16),
                pltpu.VMEM((1, feats + 128), F32),
                pltpu.VMEM((1, feats + 128), F32),
                pltpu.VMEM((1, feats + 128), F32),
                pltpu.VMEM((nd, 1, feats + 128), F32),
                pltpu.VMEM((bulk, 8, 128), F32),
                dma((6,)),
                dma, dma, dma((2,)),
                dma, dma, dma, dma, dma,
                dma((2,)), dma((2,)), dma,
                dma, dma((2,)), dma, dma((3,)), dma((2,)),
                dma, dma((2,)), dma,
            ],
            compiler_params=pltpu.CompilerParams(collective_id=0, has_side_effects=True),
        )(inputs.reshape(tokens, feats), down[0], up[0], gains, head, labels, valid)
        down_t, up_g, gain_g = pl.pallas_call(
            functools.partial(scale_kernel, part),
            out_shape=(
                jax.ShapeDtypeStruct((part, feats), F32),
                jax.ShapeDtypeStruct((part, feats), F32),
                jax.ShapeDtypeStruct((1, feats), F32),
            ),
            in_specs=[vmem],
            out_specs=(vmem,) * 3,
        )(pltpu.with_memory_space_constraint(sums, pltpu.VMEM))
        return down_t.T[None], up_g[None], gain_g

    return jax.shard_map(
        local,
        mesh=mesh,
        in_specs=(
            P(None, "dp", "tensor"),
            P("section", "tensor", None),
            P("section", None, "tensor"),
            P("section", "tensor"),
            P("tensor", None),
            P(None, "dp"),
            P(None, "dp"),
        ),
        out_specs=(
            P("section", "tensor", "dp"),
            P("section", "dp", "tensor"),
            P("section", "tensor"),
        ),
        check_vma=False,
    )
```
